256 devices in a mesh: frames: 64 (over y_hi, z, x), rows: 4 (over y_lo, core).
Axes of the slice: x: 4, y: 4 (y_hi: 2, y_lo: 2; y = y_hi * 2 + y_lo), z: 8, core: 2. Of those that a mesh axis runs over, the one named last changes fastest.
Arguments:
- video: bfloat16 [64, 32, 160, 512], P('frames', 'rows'), may hold values from -6 to 6
- norm1_gain: float32 [512], replicated, may hold values from 0.25 to 1.75
- norm1_shift: float32 [512], replicated, may hold values from -1.75 to 1.75
- conv1_weight: bfloat16 [3, 3, 512, 512], replicated, may hold values from -0.09375 to 0.09375
- conv1_bias: float32 [512], replicated, may hold values from -1.75 to 1.75
- norm2_gain: float32 [512], replicated, may hold values from 0.25 to 1.75
- norm2_shift: float32 [512], replicated, may hold values from -1.75 to 1.75
- conv2_weight: bfloat16 [3, 3, 512, 512], replicated, may hold values from -0.09375 to 0.09375
- conv2_bias: float32 [512], replicated, may hold values from -1.75 to 1.75
- out_gain: float32 [512], replicated, may hold values from 0.25 to 1.75
- out_shift: float32 [512], replicated, may hold values from -1.75 to 1.75
- out_weight: bfloat16 [3, 3, 512, 8], replicated, may hold values from -0.09375 to 0.09375
- out_bias: float32 [8], replicated, may hold values from -1.75 to 1.75
- quant_weight: float32 [8, 4], replicated, may hold values from -2 to 2
- quant_bias: float32 [4], replicated, may hold values from -1.75 to 1.75
- time_in_weight: bfloat16 [3, 3, 3, 4, 128], replicated, may hold values from -0.625 to 0.625
- time_in_bias: float32 [128], replicated, may hold values from -1.75 to 1.75
- tnorm1_gain: float32 [128], replicated, may hold values from 0.25 to 1.75
- tnorm1_shift: float32 [128], replicated, may hold values from -1.75 to 1.75
- time1_weight: bfloat16 [3, 3, 3, 128, 128], replicated, may hold values from -0.109375 to 0.109375
- tnorm2_gain: float32 [128], replicated, may hold values from 0.25 to 1.75
- tnorm2_shift: float32 [128], replicated, may hold values from -1.75 to 1.75
- time2_weight: bfloat16 [3, 3, 3, 128, 128], replicated, may hold values from -0.109375 to 0.109375
- time2_bias: float32 [128], replicated, may hold values from -1.75 to 1.75
Outputs:
- features: bfloat16 [64, 32, 160, 128], P('frames', 'rows')
The draws below stay inside these ranges and needn't reach their ends.
All inputs are finite; a program needn't handle non-finite values.
Results may differ from the reference program's by a relative error of at most 0.01.
Values may be sent and summed in bfloat16 or wider, within the bound.
A program may use at most 64 MiB of HBM per device.

```python
import jax
import jax.numpy as jnp
from jax import lax

CH = 512
LATENT = 4
TCH = 128
GROUPS = 32
WIDTH = 160
MOMENTS = 8
FRAMES = 64
HEIGHT = 32


def level_of(own_key, shape, split, least, top_value):
    gain = 1.0
    for axis_at, blocks in split:
        heights = jax.random.uniform(jax.random.fold_in(jax.random.fold_in(own_key, 6), axis_at), (blocks,), jnp.float32, least / len(split), top_value / len(split))
        gain = gain * jnp.repeat(jnp.exp(heights), shape[axis_at] // blocks).reshape((-1,) + (1,) * (len(shape) - 1 - axis_at))
    return gain


def scatter_about(key, dims, width, most, pieces=(), kind=jnp.bfloat16):
    values = width * jax.random.normal(key, dims, jnp.float32)
    if pieces:
        values = values * level_of(key, dims, pieces, -0.22, 0.18)
    return jnp.clip(values, -most, most).astype(kind)


def setup_inputs(seed: int = 0) -> dict:
    splits = jax.random.split(jax.random.key(seed), 25)
    return {
        "video": scatter_about(splits[0], (FRAMES, HEIGHT, WIDTH, CH), 1.0, 6.0, ((0, 64), (1, 4))),
        "norm1_gain": jnp.clip(1.0 + 0.15 * jax.random.normal(splits[1], (CH,), jnp.float32), 0.25, 1.75),
        "norm1_shift": scatter_about(splits[2], (CH,), 0.3, 1.75, (), jnp.float32),
        "conv1_weight": scatter_about(splits[3], (3, 3, CH, CH), (9 * CH) ** -0.5, 0.09375),
        "conv1_bias": scatter_about(splits[4], (CH,), 0.3, 1.75, (), jnp.float32),
        "norm2_gain": jnp.clip(1.0 + 0.15 * jax.random.normal(splits[5], (CH,), jnp.float32), 0.25, 1.75),
        "norm2_shift": scatter_about(splits[6], (CH,), 0.3, 1.75, (), jnp.float32),
        "conv2_weight": scatter_about(splits[7], (3, 3, CH, CH), (9 * CH) ** -0.5, 0.09375),
        "conv2_bias": scatter_about(splits[8], (CH,), 0.3, 1.75, (), jnp.float32),
        "out_gain": jnp.clip(1.0 + 0.15 * jax.random.normal(splits[9], (CH,), jnp.float32), 0.25, 1.75),
        "out_shift": scatter_about(splits[10], (CH,), 0.3, 1.75, (), jnp.float32),
        "out_weight": scatter_about(splits[11], (3, 3, CH, MOMENTS), (9 * CH) ** -0.5, 0.09375),
        "out_bias": scatter_about(splits[12], (MOMENTS,), 0.3, 1.75, (), jnp.float32),
        "quant_weight": scatter_about(splits[13], (MOMENTS, LATENT), MOMENTS ** -0.5, 2.0, (), jnp.float32),
        "quant_bias": scatter_about(splits[14], (LATENT,), 0.3, 1.75, (), jnp.float32),
        "time_in_weight": scatter_about(splits[15], (3, 3, 3, LATENT, TCH), (27 * LATENT) ** -0.5, 0.625),
        "time_in_bias": scatter_about(splits[16], (TCH,), 0.3, 1.75, (), jnp.float32),
        "tnorm1_gain": jnp.clip(1.0 + 0.15 * jax.random.normal(splits[17], (TCH,), jnp.float32), 0.25, 1.75),
        "tnorm1_shift": scatter_about(splits[18], (TCH,), 0.3, 1.75, (), jnp.float32),
        "time1_weight": scatter_about(splits[19], (3, 3, 3, TCH, TCH), (27 * TCH) ** -0.5, 0.109375),
        "tnorm2_gain": jnp.clip(1.0 + 0.15 * jax.random.normal(splits[20], (TCH,), jnp.float32), 0.25, 1.75),
        "tnorm2_shift": scatter_about(splits[21], (TCH,), 0.3, 1.75, (), jnp.float32),
        "time2_weight": scatter_about(splits[22], (3, 3, 3, TCH, TCH), (27 * TCH) ** -0.5, 0.109375),
        "time2_bias": scatter_about(splits[23], (TCH,), 0.3, 1.75, (), jnp.float32),
    }


EPS = 1e-06
LATENT_SCALE = 0.13025

def group_act(values, norm_gain, norm_shift):
    shape = values.shape
    grouped = values.reshape(shape[0], shape[1] * shape[2], GROUPS, shape[3] // GROUPS)
    axes = (1, 3)
    average = lax.optimization_barrier(jnp.mean(grouped, axis=axes, keepdims=True))
    centred = grouped - average
    variance = lax.optimization_barrier(jnp.mean(centred * centred, axis=axes, keepdims=True))
    scaled = (centred * lax.rsqrt(variance + EPS)).reshape(shape)
    return jax.nn.silu(scaled * norm_gain + norm_shift).astype(jnp.bfloat16)

def plane_conv(active, weight, offset):
    height, columns, channels = (active.shape[1], active.shape[2], active.shape[3])

    def one_frame(current):
        padded = jnp.pad(current, ((1, 1), (1, 1), (0, 0)))
        summed = jnp.zeros((height * columns, weight.shape[3]), jnp.float32)
        for row_off in range(3):
            for col_off in range(3):
                window = padded[row_off:row_off + height, col_off:col_off + columns].reshape(-1, channels)
                summed = summed + jnp.dot(window, weight[row_off, col_off], preferred_element_type=jnp.float32)
        return summed.reshape(height, columns, -1) + offset
    return lax.map(one_frame, active)

def clip_conv(active, weight, offset):
    count, height, columns, channels = active.shape
    padded = jnp.pad(active, ((2, 0), (1, 1), (1, 1), (0, 0)))
    summed = jnp.zeros((count * height * columns, weight.shape[4]), jnp.float32)
    for time_off in range(3):
        for row_off in range(3):
            for col_off in range(3):
                window = padded[time_off:time_off + count, row_off:row_off + height, col_off:col_off + columns]
                summed = summed + jnp.dot(window.reshape(-1, channels), weight[time_off, row_off, col_off], preferred_element_type=jnp.float32)
    return summed.reshape(count, height, columns, -1) + offset

def reference(video, norm1_gain, norm1_shift, conv1_weight, conv1_bias, norm2_gain, norm2_shift, conv2_weight, conv2_bias, out_gain, out_shift, out_weight, out_bias, quant_weight, quant_bias, time_in_weight, time_in_bias, tnorm1_gain, tnorm1_shift, time1_weight, tnorm2_gain, tnorm2_shift, time2_weight, time2_bias):
    inputs = video.astype(jnp.float32)
    first_act = group_act(inputs, norm1_gain, norm1_shift)
    hidden = plane_conv(first_act, conv1_weight, conv1_bias)
    second_act = group_act(hidden, norm2_gain, norm2_shift)
    block_out = inputs + plane_conv(second_act, conv2_weight, conv2_bias)
    head_act = group_act(block_out, out_gain, out_shift)
    moments = plane_conv(head_act, out_weight, out_bias)
    shape = moments.shape
    means = jnp.dot(moments.reshape(-1, shape[3]), quant_weight, precision=lax.Precision.HIGHEST) + quant_bias
    latent = (LATENT_SCALE * means).astype(jnp.bfloat16).reshape(shape[0], shape[1], shape[2], -1)
    lifted = clip_conv(latent, time_in_weight, time_in_bias)
    time_act = group_act(lifted, tnorm1_gain, tnorm1_shift)
    inner = clip_conv(time_act, time1_weight, 0.0)
    last_act = group_act(inner, tnorm2_gain, tnorm2_shift)
    return (lifted + clip_conv(last_act, time2_weight, time2_bias)).astype(jnp.bfloat16)
```

```python
import functools

import jax
import jax.numpy as jnp
from jax import lax
from jax.experimental import pallas as pl
from jax.experimental.pallas import tpu as pltpu
from jax.sharding import PartitionSpec as P

GROUPS = 32
EPS = 1e-06
LATENT_SCALE = 0.13025

R = 8
W = 160
C = 512
T = 128
LANES = 256
BACK = 6

MESH = pl.DeviceIdType.MESH
F32 = jnp.float32
BF16 = jnp.bfloat16


def lane_group_sum(x, size):
    lane = lax.broadcasted_iota(jnp.int32, x.shape, 1)
    step = 1
    while step < size:
        up = pltpu.roll(x, step, 1)
        down = pltpu.roll(x, 128 - step, 1)
        x = x + jnp.where((lane // step) % 2 == 1, up, down)
        step *= 2
    return x


def column_shifts(a):
    col = lax.broadcasted_iota(jnp.int32, a.shape, 0)
    left = jnp.where(col == 0, 0.0, pltpu.roll(a, 1, 0))
    right = jnp.where(col == W - 1, 0.0, pltpu.roll(a, W - 1, 0))
    return left.astype(BF16), a.astype(BF16), right.astype(BF16)


def half_silu(v, scale, shift):
    w = v * scale + shift
    return w * jnp.tanh(w) + w


def partial_sums(v):
    g = v.reshape(-1, 8, v.shape[-1])
    return jnp.sum(g, axis=0), jnp.sum(g * g, axis=0)


def kernel(
    n_frames,
    n_rows,
    video, g1, s1, cw1, cb1, g2, s2, cw2, cb2, g3, s3, ow, ob, qw, qb,
    tiw, tib, tg1, ts1, tw1, tg2, ts2, tw2, tb2,
    out,
    vid, w1, w2, act, h, hsend, hrecv, ysend, yrecv,
    params, cbias, tparams, obv, qwv, qbv, tiwv,
    wht, pt, mom, wbf, wb, w1r, w2r,
    stbuf, tstbuf, latsend, lx, ltt, t0s, b1, t1s, b2, outv,
    in_sem, vh_sem, hh_sem, yh_sem, st_sem, lat_send, lat_recv,
):
    f = lax.axis_index("frames")
    rr = lax.axis_index("rows")

    def local(src, dst, k):
        return pltpu.make_async_copy(src, dst, in_sem.at[k])

    c_vid = local(video, vid.at[pl.ds(1, R)], 0)
    c_w1 = local(cw1, w1, 1)
    c_w2 = local(cw2, w2, 2)
    c_par = [local(a, params.at[i], 3 + i) for i, a in enumerate((g1, s1, g2, s2, g3, s3))]
    c_cb = [local(a, cbias.at[i], 9 + i) for i, a in enumerate((cb1, cb2))]
    c_tp = [local(a, tparams.at[i], 11 + i) for i, a in enumerate((tib, tg1, ts1, tg2, ts2, tb2))]
    c_ow = local(ow, wht, 17)
    c_q = [local(ob, obv, 18), local(qw, qwv, 19), local(qb, qbv, 20)]
    c_tiw = local(tiw, tiwv, 21)
    c_t = []
    for i, (src, dst) in enumerate(((tw1, w1r), (tw2, w2r))):
        for p in range(2):
            c_t.append(local(src, dst.at[:, pl.ds(p, 3), :, pl.ds(T * p, T)], 22 + 2 * i + p))

    def begin(copies):
        for c in copies:
            c.start()

    def finish(copies):
        for c in copies:
            c.wait()

    def lat_targets():
        for k in range(BACK + 1):
            for d in (-1, 0, 1):
                if k or d:
                    yield k, d

    def sends_to(k, d):
        ok = f + k < n_frames
        if d == -1:
            ok = jnp.logical_and(ok, rr > 0)
        if d == 1:
            ok = jnp.logical_and(ok, rr < n_rows - 1)
        return ok

    def gets_from(k, d):
        ok = f >= k
        if d == -1:
            ok = jnp.logical_and(ok, rr < n_rows - 1)
        if d == 1:
            ok = jnp.logical_and(ok, rr > 0)
        return ok

    c_vid.start()
    barrier = pltpu.get_barrier_semaphore()
    for d in range(1, n_rows):
        pl.semaphore_signal(
            barrier, inc=1, device_id={"frames": f, "rows": lax.rem(rr + d, n_rows)},
            device_id_type=MESH,
        )
    for k, d in lat_targets():
        if k:
            @pl.when(gets_from(k, d))
            def _():
                pl.semaphore_signal(
                    barrier, inc=1, device_id={"frames": f - k, "rows": rr - d}, device_id_type=MESH
                )

    begin(c_par + c_cb + c_tp + [c_ow] + c_q + [c_tiw])

    def halo(src_last, src_first, dst_above, dst_below, sem):
        down = pltpu.make_async_remote_copy(
            src_ref=src_last, dst_ref=dst_above, send_sem=sem.at[0], recv_sem=sem.at[1],
            device_id={"frames": f, "rows": rr + 1}, device_id_type=MESH,
        )
        up = pltpu.make_async_remote_copy(
            src_ref=src_first, dst_ref=dst_below, send_sem=sem.at[2], recv_sem=sem.at[3],
            device_id={"frames": f, "rows": rr - 1}, device_id_type=MESH,
        )
        return down, up

    has_above = rr > 0
    has_below = rr < n_rows - 1

    def stat_copies(buf, e):
        return [
            pltpu.make_async_remote_copy(
                src_ref=buf.at[rr], dst_ref=buf.at[rr],
                send_sem=st_sem.at[e, 0, d - 1], recv_sem=st_sem.at[e, 1, d - 1],
                device_id={"frames": f, "rows": lax.rem(rr + d, n_rows)}, device_id_type=MESH,
            )
            for d in range(1, n_rows)
        ]

    def send_stats(e, s, q):
        s = jnp.sum(s, axis=0, keepdims=True)
        q = jnp.sum(q, axis=0, keepdims=True)
        for t in range(C // 128):
            stbuf[e, rr, t : t + 1, :] = s[:, 128 * t : 128 * t + 128]
            stbuf[e, rr, 4 + t : 5 + t, :] = q[:, 128 * t : 128 * t + 128]
        copies = stat_copies(stbuf.at[e], e)
        begin(copies)
        return copies

    def norm_terms(e, copies, gain, shift):
        finish(copies)
        total = stbuf[e, 0]
        for r in range(1, n_rows):
            total = total + stbuf[e, r]
        total = lane_group_sum(total, C // GROUPS) * (1.0 / (n_rows * R * W * (C // GROUPS)))
        mean = total[0:4]
        var = jnp.maximum(total[4:8] - mean * mean, 0.0)
        scale = lax.rsqrt(var + EPS) * gain
        shift = shift - mean * scale
        wide = lambda x: jnp.concatenate([x[t : t + 1] for t in range(C // 128)], axis=1) * 0.5
        return wide(scale), wide(shift)

    def put_line(line, v, scale, shift, shifted=True):
        a = half_silu(v, scale, shift)
        if shifted:
            for j, x in enumerate(column_shifts(a)):
                act[j, line] = x
        else:
            act[1, line] = a.astype(BF16)

    def halo_lines(copies, above, below, scale, shift, shifted=True):
        taps = range(3) if shifted else (1,)
        for has, copy, ref, line in (
            (has_above, copies[0], above, 0),
            (has_below, copies[1], below, R + 1),
        ):
            @pl.when(has)
            def _():
                copy.wait_recv()
                put_line(line, ref[...].astype(F32), scale, shift, shifted)

            @pl.when(jnp.logical_not(has))
            def _():
                for j in taps:
                    act[j, line] = jnp.zeros((W, C), BF16)

    def start_down(copies):
        @pl.when(has_below)
        def _():
            copies[0].start()

    def start_up(copies):
        @pl.when(has_above)
        def _():
            copies[1].start()

    def end_sends(copies):
        @pl.when(has_below)
        def _():
            copies[0].wait_send()

        @pl.when(has_above)
        def _():
            copies[1].wait_send()

    def conv(weight, finish_line):
        def block(b, carry):
            s, q = carry
            lo = 2 * b
            hi = R - 2 - 2 * b
            acc = None
            for i in range(3):
                for j in range(3):
                    lhs = jnp.concatenate(
                        [
                            act[j, pl.ds(lo + i, 2)].reshape(2 * W, C),
                            act[j, pl.ds(hi + i, 2)].reshape(2 * W, C),
                        ],
                        axis=0,
                    )
                    d = jnp.dot(lhs, weight[3 * i + j], preferred_element_type=F32)
                    acc = d if acc is None else acc + d
            return finish_line(b, lo, hi, acc, s, q)

        zero = jnp.zeros((8, C), F32)
        return lax.fori_loop(0, 2, block, (zero, zero))

    tstbuf[...] = jnp.zeros(tstbuf.shape, F32)
    c_vid.wait()
    c_w1.start()

    def video_sums(r, carry):
        s, q = carry
        a, b = partial_sums(vid[r + 1].astype(F32))
        return s + a, q + b

    zero = jnp.zeros((8, C), F32)
    s, q = lax.fori_loop(0, R, video_sums, (zero, zero))

    later = sum(1 - lax.div(f + k, n_frames) for k in range(1, BACK + 1))
    lines = 2 + lax.div(rr + n_rows - 1, n_rows) - lax.div(rr + 1, n_rows)
    pl.semaphore_wait(barrier, n_rows - 1 + later * lines)

    copies = send_stats(0, s, q)
    vh = halo(vid.at[R], vid.at[1], vid.at[0], vid.at[R + 1], vh_sem)
    start_down(vh)
    start_up(vh)
    c_w2.start()
    begin(c_t)

    finish([c_tiw])
    wbf[...] = jnp.zeros(wbf.shape, F32)
    for t in range(3):
        for j in range(3):
            for i in range(3):
                piece = tiwv[t, i, j].astype(F32)
                for n in range(R + 4):
                    top = 64 * j + 4 * (n + 1 + i)
                    wbf[top : top + 4, T * n : T * n + T] = piece
        for n in range(3):
            wb[n, 256 * t : 256 * t + 256] = wbf[:, 512 * n : 512 * n + 512].astype(BF16)

    finish(c_par + c_cb)
    scale, shift = norm_terms(0, copies, params[0], params[1])

    def video_line(r, _):
        put_line(r + 1, vid[r + 1].astype(F32), scale, shift)
        return 0

    lax.fori_loop(0, R, video_line, 0)
    halo_lines(vh, vid.at[0], vid.at[R + 1], scale, shift)
    c_w1.wait()

    hh = halo(hsend.at[1], hsend.at[0], hrecv.at[0], hrecv.at[1], hh_sem)

    def h_lines(b, lo, hi, acc, s, q):
        v = acc + cbias[0]
        h[pl.ds(lo, 2)] = v[: 2 * W].reshape(2, W, C)
        h[pl.ds(hi, 2)] = v[2 * W :].reshape(2, W, C)

        @pl.when(b == 0)
        def _():
            hsend[0] = v[:W].astype(BF16)
            hsend[1] = v[3 * W :].astype(BF16)
            start_down(hh)
            start_up(hh)

        a, c = partial_sums(v)
        return s + a, q + c

    s, q = conv(w1, h_lines)
    copies = send_stats(1, s, q)

    finish([c_ow] + c_q + c_tp)
    nt = (((1,), (1,)), ((), ()))
    pt[...] = jnp.zeros(pt.shape, F32)
    for t in range(3):
        for dst in (w1r, w2r):
            dst[t, 3, :, 0:T] = jnp.zeros((3 * T, T), BF16)
            dst[t, 0, :, T : 2 * T] = jnp.zeros((3 * T, T), BF16)
    row = lax.broadcasted_iota(jnp.int32, (4 * R, 8 * R), 0)
    col = lax.broadcasted_iota(jnp.int32, (4 * R, 8 * R), 1)
    quant = jnp.zeros((4 * R, 8 * R), F32)
    for m in range(8):
        for c in range(4):
            hit = (row % 4 == c) & (col % 8 == m) & (row // 4 == col // 8)
            quant = quant + jnp.where(hit, qwv[c : c + 1, m : m + 1], 0.0)
    row8 = lax.broadcasted_iota(jnp.int32, (8 * R, 1), 0)
    row4 = lax.broadcasted_iota(jnp.int32, (4 * R, 1), 0)
    head_bias = jnp.zeros((8 * R, 1), F32)
    for m in range(8):
        head_bias = head_bias + jnp.where(row8 % 8 == m, obv[0:1, m : m + 1], 0.0)
    quant_bias = jnp.zeros((4 * R, 1), F32)
    for c in range(4):
        quant_bias = quant_bias + jnp.where(row4 % 4 == c, qbv[0:1, c : c + 1], 0.0)

    scale, shift = norm_terms(1, copies, params[2], params[3])

    def h_line(r, _):
        put_line(r + 1, h[r], scale, shift)
        return 0

    lax.fori_loop(0, R, h_line, 0)
    halo_lines(hh, hrecv.at[0], hrecv.at[1], scale, shift)
    c_w2.wait()

    yh = halo(ysend.at[1], ysend.at[0], yrecv.at[0], yrecv.at[1], yh_sem)

    def y_lines(b, lo, hi, acc, s, q):
        res = jnp.concatenate(
            [vid[pl.ds(lo + 1, 2)].reshape(2 * W, C), vid[pl.ds(hi + 1, 2)].reshape(2 * W, C)],
            axis=0,
        )
        v = res.astype(F32) + (acc + cbias[1])
        h[pl.ds(lo, 2)] = v[: 2 * W].reshape(2, W, C)
        h[pl.ds(hi, 2)] = v[2 * W :].reshape(2, W, C)

        @pl.when(b == 0)
        def _():
            ysend[0] = v[:W].astype(BF16)
            ysend[1] = v[3 * W :].astype(BF16)
            start_down(yh)
            start_up(yh)

        a, c = partial_sums(v)
        return s + a, q + c

    s, q = conv(w2, y_lines)
    copies = send_stats(2, s, q)
    scale, shift = norm_terms(2, copies, params[4], params[5])

    def y_line(r, _):
        put_line(r + 1, h[r], scale, shift, shifted=False)
        return 0

    lax.fori_loop(0, R, y_line, 0)
    halo_lines(yh, yrecv.at[0], yrecv.at[1], scale, shift, shifted=False)

    for r in range(R + 2):
        pt[r, :, 0:W] = lax.dot_general(wht[...], act[1, r], nt, preferred_element_type=F32)
    for r in range(R):
        sums = []
        for j in range(3):
            x = None
            for i in range(3):
                top = 8 * (3 * i + j)
                p = pt[r + i, top : top + 8, :]
                x = p if x is None else x + p
            sums.append(x)
        mom[8 * r : 8 * r + 8] = (
            sums[1] + pltpu.roll(sums[0], 1, 1) + pltpu.roll(sums[2], LANES - 1, 1)
        )
    means = (
        jnp.dot(quant, mom[...] + head_bias, precision=lax.Precision.HIGHEST, preferred_element_type=F32)
        + quant_bias
    )
    inside = lax.broadcasted_iota(jnp.int32, means.shape, 1) < W
    latent = jnp.where(inside, LATENT_SCALE * means, 0.0).astype(BF16)
    latsend[...] = latent
    lx[0, 16:48] = latent

    def lat_copy(k, d):
        src = {0: latsend, 1: latsend.at[pl.ds(16, 16)], -1: latsend.at[pl.ds(0, 16)]}[d]
        at = {0: pl.ds(16, 32), 1: pl.ds(0, 16), -1: pl.ds(48, 16)}[d]
        return pltpu.make_async_remote_copy(
            src_ref=src, dst_ref=lx.at[k, at],
            send_sem=lat_send.at[k, d + 1], recv_sem=lat_recv.at[k, d + 1],
            device_id={"frames": f + k, "rows": rr + d}, device_id_type=MESH,
        )

    for k, d in lat_targets():
        @pl.when(sends_to(k, d))
        def _():
            lat_copy(k, d).start()

    line16 = lax.broadcasted_iota(jnp.int32, (64, LANES), 0) // 16
    for k in range(BACK + 1):
        for d in (-1, 0, 1):
            if k or d:
                @pl.when(gets_from(k, d))
                def _():
                    lat_copy(k, d).wait_recv()
        lowest = jnp.where(has_above, 0, 1)
        highest = jnp.where(has_below, 4, 3)
        lowest = jnp.where(f >= k, lowest, 4)
        keep = (line16 >= lowest) & (line16 < highest)
        x = jnp.where(keep, lx[k].astype(F32), 0.0)
        stack = jnp.concatenate(
            [pltpu.roll(x, 1, 1), x, pltpu.roll(x, LANES - 1, 1), jnp.zeros((64, LANES), F32)],
            axis=0,
        )
        ltt[k] = jnp.transpose(stack)[:W].astype(BF16)

    finish(c_t)
    n_g = 5
    sums = [[jnp.zeros((8, T), F32), jnp.zeros((8, T), F32)] for _ in range(n_g)]
    for n in range(3):
        lhs = jnp.concatenate(
            [
                jnp.concatenate([ltt[g + 2], ltt[g + 1], ltt[g]], axis=1)
                for g in range(n_g)
            ],
            axis=0,
        )
        acc = jnp.dot(lhs, wb[n], preferred_element_type=F32)
        for g in range(n_g):
            for m in range(4):
                v = acc[W * g : W * g + W, T * m : T * m + T] + tparams[0]
                t0s[g, 4 * n + m] = v
                if 2 <= 4 * n + m < R + 2:
                    a, c = partial_sums(v)
                    sums[g][0] += a
                    sums[g][1] += c

    def send_time_stats(e, sums):
        for i, (s, q) in enumerate(sums):
            tstbuf[e, rr, 2 * i : 2 * i + 1] = jnp.sum(s, axis=0, keepdims=True)
            tstbuf[e, rr, 2 * i + 1 : 2 * i + 2] = jnp.sum(q, axis=0, keepdims=True)
        copies = stat_copies(tstbuf.at[e], 3 + e)
        begin(copies)
        return copies

    def time_terms(e, copies, count, gain, shift):
        finish(copies)
        total = tstbuf[e, 0]
        for r in range(1, n_rows):
            total = total + tstbuf[e, r]
        total = lane_group_sum(total, T // GROUPS) * (1.0 / (n_rows * R * W * (T // GROUPS)))
        terms = []
        for i in range(count):
            mean = total[2 * i : 2 * i + 1]
            var = jnp.maximum(total[2 * i + 1 : 2 * i + 2] - mean * mean, 0.0)
            scale = lax.rsqrt(var + EPS) * gain
            terms.append((0.5 * scale, 0.5 * (shift - mean * scale)))
        return terms

    def time_lines(src, dst, n_lines, margin, terms):
        def line(n, _):
            at = R * rr + n - margin
            in_frame = jnp.logical_and(at >= 0, at < n_rows * R)
            for g, (scale, shift) in enumerate(terms):
                ok = jnp.logical_and(in_frame, f >= g)
                a = half_silu(src[g, n], scale, shift)
                a = jnp.where(ok, a, 0.0)
                for j, x in enumerate(column_shifts(a)):
                    dst[g, n, :, T * j : T * j + T] = x
            return 0

        lax.fori_loop(0, n_lines, line, 0)

    def pair_sums(src, weight, g, pairs):
        acc = None
        for t in range(3):
            for i in range(4):
                lhs = jnp.concatenate([src[g + 2 - t, 2 * p + i] for p in range(pairs)], axis=0)
                d = jnp.dot(lhs, weight[t, i], preferred_element_type=F32)
                acc = d if acc is None else acc + d
        return acc

    copies = send_time_stats(0, sums)
    terms = time_terms(0, copies, n_g, tparams[1], tparams[2])
    time_lines(t0s, b1, R + 4, 2, terms)

    sums = []
    for g in range(3):
        acc = pair_sums(b1, w1r, g, R // 2 + 1)
        s = jnp.zeros((8, T), F32)
        q = jnp.zeros((8, T), F32)
        for p in range(R // 2 + 1):
            for half in range(2):
                v = acc[W * p : W * p + W, T * half : T * half + T]
                t1s[g, 2 * p + half] = v
                if 1 <= 2 * p + half < R + 1:
                    a, c = partial_sums(v)
                    s += a
                    q += c
        sums.append((s, q))
    copies = send_time_stats(1, sums)
    terms = time_terms(1, copies, 3, tparams[3], tparams[4])
    time_lines(t1s, b2, R + 2, 1, terms)

    acc = pair_sums(b2, w2r, 0, R // 2)
    for p in range(R // 2):
        for half in range(2):
            v = acc[W * p : W * p + W, T * half : T * half + T] + tparams[5]
            outv[2 * p + half] = (t0s[0, 2 * p + half + 2] + v).astype(BF16)
    c_out = local(outv, out, 0)
    c_out.start()
    end_sends(vh)
    end_sends(hh)
    end_sends(yh)
    for k, d in lat_targets():
        @pl.when(sends_to(k, d))
        def _():
            lat_copy(k, d).wait_send()
    c_out.wait()


def body(
    video, norm1_gain, norm1_shift, conv1_weight, conv1_bias, norm2_gain, norm2_shift,
    conv2_weight, conv2_bias, out_gain, out_shift, out_weight, out_bias, quant_weight,
    quant_bias, time_in_weight, time_in_bias, tnorm1_gain, tnorm1_shift, time1_weight,
    tnorm2_gain, tnorm2_shift, time2_weight, time2_bias, *, n_frames, n_rows,
):
    tile = lambda a: a.reshape(4, 128)
    flat = lambda a: a.reshape(1, -1)
    args = (
        video.reshape(R, W, C),
        tile(norm1_gain), tile(norm1_shift), conv1_weight.reshape(9, C, C), flat(conv1_bias),
        tile(norm2_gain), tile(norm2_shift), conv2_weight.reshape(9, C, C), flat(conv2_bias),
        tile(out_gain), tile(out_shift), out_weight.transpose(0, 1, 3, 2).reshape(72, C), flat(out_bias),
        quant_weight.T, flat(quant_bias), time_in_weight, flat(time_in_bias),
        flat(tnorm1_gain), flat(tnorm1_shift), time1_weight.reshape(3, 3, 3 * T, T),
        flat(tnorm2_gain), flat(tnorm2_shift), time2_weight.reshape(3, 3, 3 * T, T),
        flat(time2_bias),
    )
    vmem = lambda *shape, dtype=BF16: pltpu.VMEM(shape, dtype)
    dma = pltpu.SemaphoreType.DMA
    result = pl.pallas_call(
        functools.partial(kernel, n_frames, n_rows),
        out_shape=jax.ShapeDtypeStruct((R, W, T), BF16),
        in_specs=[pl.BlockSpec(memory_space=pl.ANY)] * len(args),
        out_specs=pl.BlockSpec(memory_space=pl.ANY),
        scratch_shapes=[
            vmem(R + 2, W, C),
            vmem(9, C, C),
            vmem(9, C, C),
            vmem(3, R + 2, W, C),
            vmem(R, W, C, dtype=F32),
            vmem(2, W, C),
            vmem(2, W, C),
            vmem(2, W, C),
            vmem(2, W, C),
            vmem(6, 4, 128, dtype=F32),
            vmem(2, 1, C, dtype=F32),
            vmem(6, 1, T, dtype=F32),
            vmem(1, 8, dtype=F32),
            vmem(4, 8, dtype=F32),
            vmem(1, 4, dtype=F32),
            vmem(3, 3, 3, 4, T),
            vmem(72, C),
            vmem(R + 2, 72, LANES, dtype=F32),
            vmem(8 * R, LANES, dtype=F32),
            vmem(256, 12 * T, dtype=F32),
            vmem(3, 768, 4 * T),
            vmem(3, 4, 3 * T, 2 * T),
            vmem(3, 4, 3 * T, 2 * T),
            vmem(3, n_rows, 8, 128, dtype=F32),
            vmem(2, n_rows, 16, 128, dtype=F32),
            vmem(4 * R, LANES),
            vmem(BACK + 1, 64, LANES),
            vmem(BACK + 1, W, 256),
            vmem(5, R + 4, W, T, dtype=F32),
            vmem(5, R + 4, W, 3 * T),
            vmem(3, R + 2, W, T, dtype=F32),
            vmem(3, R + 2, W, 3 * T),
            vmem(R, W, T),
            dma((26,)),
            dma((4,)),
            dma((4,)),
            dma((4,)),
            dma((5, 2, n_rows - 1)),
            dma((BACK + 1, 3)),
            dma((BACK + 1, 3)),
        ],
        compiler_params=pltpu.CompilerParams(
            collective_id=0, has_side_effects=True, vmem_limit_bytes=62 * 1024 * 1024
        ),
        name="encoder_window",
    )(*args)
    return result[None]


def solution(mesh):
    step = functools.partial(body, n_frames=mesh.shape["frames"], n_rows=mesh.shape["rows"])
    return jax.shard_map(
        step,
        mesh=mesh,
        in_specs=(P("frames", "rows", None, None),) + (P(),) * 23,
        out_specs=P("frames", "rows", None, None),
        check_vma=False,
    )
```

```python
import functools

import jax
import jax.numpy as jnp
from jax import lax
from jax.experimental import pallas as pl
from jax.experimental.pallas import tpu as pltpu
from jax.sharding import PartitionSpec as P

GROUPS = 32
EPS = 1e-06
LATENT_SCALE = 0.13025

R = 8
W = 160
C = 512
T = 128
HALF = C // 2
LANES = 256
BACK = 6

MESH = pl.DeviceIdType.MESH
F32 = jnp.float32
BF16 = jnp.bfloat16


def lane_group_sum(x, size):
    lane = lax.broadcasted_iota(jnp.int32, x.shape, 1)
    step = 1
    while step < size:
        up = pltpu.roll(x, step, 1)
        down = pltpu.roll(x, 128 - step, 1)
        x = x + jnp.where((lane // step) % 2 == 1, up, down)
        step *= 2
    return x


def column_shifts(a):
    col = lax.broadcasted_iota(jnp.int32, a.shape, 0)
    left = jnp.where(col == 0, 0.0, pltpu.roll(a, 1, 0))
    right = jnp.where(col == W - 1, 0.0, pltpu.roll(a, W - 1, 0))
    return left.astype(BF16), a.astype(BF16), right.astype(BF16)


def half_silu(v, scale, shift):
    w = v * scale + shift
    return w * jnp.tanh(w) + w


def partial_sums(v):
    g = v.reshape(-1, 8, v.shape[-1])
    return jnp.sum(g, axis=0), jnp.sum(g * g, axis=0)


def kernel(
    n_frames,
    n_rows,
    video, g1, s1, cw1, cb1, g2, s2, cw2, cb2, g3, s3, ow, ob, qw, qb,
    tiw, tib, tg1, ts1, tw1, tg2, ts2, tw2, tb2,
    out,
    vid, w1, w2, act, h, yp, hsend, hrecv, ysend, yrecv,
    params, cbias, tparams, obv, qwv, qbv, tiwv,
    wht, pt, mom, wbf, wb, w1r, w2r,
    stbuf, tstbuf, latsend, lx, ltt, t0s, b1, t1s, b2, facc,
    in_sem, vh_sem, hh_sem, yh_sem, st_sem, lat_send, lat_recv,
):
    f = lax.axis_index("frames")
    rr = lax.axis_index("rows")

    def local(src, dst, k):
        return pltpu.make_async_copy(src, dst, in_sem.at[k])

    c_vid = local(video, vid.at[pl.ds(1, R)], 0)
    c_w1 = [local(cw1.at[:, :, pl.ds(HALF * i, HALF)], w1.at[i], (1, 26)[i]) for i in range(2)]
    c_w2 = local(cw2, w2, 2)
    c_par = [local(a, params.at[i], 3 + i) for i, a in enumerate((g1, s1, g2, s2, g3, s3))]
    c_cb = [local(a, cbias.at[i], 9 + i) for i, a in enumerate((cb1, cb2))]
    c_tp = [local(a, tparams.at[i], 11 + i) for i, a in enumerate((tib, tg1, ts1, tg2, ts2, tb2))]
    c_ow = local(ow, wht, 17)
    c_q = [local(ob, obv, 18), local(qw, qwv, 19), local(qb, qbv, 20)]
    c_tiw = local(tiw, tiwv, 21)
    c_t = []
    for i, (src, dst) in enumerate(((tw1, w1r), (tw2, w2r))):
        for p in range(2):
            c_t.append(local(src, dst.at[:, pl.ds(p, 3), :, pl.ds(T * p, T)], 22 + 2 * i + p))

    def begin(copies):
        for c in copies:
            c.start()

    def finish(copies):
        for c in copies:
            c.wait()

    def lat_targets():
        for k in range(BACK + 1):
            for d in (-1, 0, 1):
                if k or d:
                    yield k, d

    def sends_to(k, d):
        ok = f + k < n_frames
        if d == -1:
            ok = jnp.logical_and(ok, rr > 0)
        if d == 1:
            ok = jnp.logical_and(ok, rr < n_rows - 1)
        return ok

    def gets_from(k, d):
        ok = f >= k
        if d == -1:
            ok = jnp.logical_and(ok, rr < n_rows - 1)
        if d == 1:
            ok = jnp.logical_and(ok, rr > 0)
        return ok

    c_vid.start()
    stbuf[...] = jnp.zeros(stbuf.shape, F32)
    tstbuf[...] = jnp.zeros(tstbuf.shape, F32)
    barrier = pltpu.get_barrier_semaphore()
    for d in range(1, n_rows):
        pl.semaphore_signal(
            barrier, inc=1, device_id={"frames": f, "rows": lax.rem(rr + d, n_rows)},
            device_id_type=MESH,
        )
    for k, d in lat_targets():
        if k:
            @pl.when(gets_from(k, d))
            def _():
                pl.semaphore_signal(
                    barrier, inc=1, device_id={"frames": f - k, "rows": rr - d}, device_id_type=MESH
                )

    begin(c_par + c_cb + c_tp + [c_ow] + c_q + [c_tiw])

    def halo(src_last, src_first, dst_above, dst_below, sem):
        down = pltpu.make_async_remote_copy(
            src_ref=src_last, dst_ref=dst_above, send_sem=sem.at[0], recv_sem=sem.at[1],
            device_id={"frames": f, "rows": rr + 1}, device_id_type=MESH,
        )
        up = pltpu.make_async_remote_copy(
            src_ref=src_first, dst_ref=dst_below, send_sem=sem.at[2], recv_sem=sem.at[3],
            device_id={"frames": f, "rows": rr - 1}, device_id_type=MESH,
        )
        return down, up

    has_above = rr > 0
    has_below = rr < n_rows - 1

    def stat_copies(buf, e):
        return [
            pltpu.make_async_remote_copy(
                src_ref=buf.at[rr], dst_ref=buf.at[rr],
                send_sem=st_sem.at[e, 0, d - 1], recv_sem=st_sem.at[e, 1, d - 1],
                device_id={"frames": f, "rows": lax.rem(rr + d, n_rows)}, device_id_type=MESH,
            )
            for d in range(1, n_rows)
        ]

    def send_stats(e, s, q):
        s = jnp.sum(s, axis=0, keepdims=True)
        q = jnp.sum(q, axis=0, keepdims=True)
        tiles = s.shape[1] // 128
        for t in range(tiles):
            stbuf[e, rr, t : t + 1, :] = s[:, 128 * t : 128 * t + 128]
            stbuf[e, rr, tiles + t : tiles + t + 1, :] = q[:, 128 * t : 128 * t + 128]
        copies = stat_copies(stbuf.at[e], e)
        begin(copies)
        return copies

    def norm_terms(e, copies, gain, shift):
        finish(copies)
        tiles = gain.shape[0]
        total = stbuf[e, 0]
        for r in range(1, n_rows):
            total = total + stbuf[e, r]
        total = lane_group_sum(total, C // GROUPS) * (1.0 / (n_rows * R * W * (C // GROUPS)))
        mean = total[0:tiles]
        var = jnp.maximum(total[tiles : 2 * tiles] - mean * mean, 0.0)
        scale = lax.rsqrt(var + EPS) * gain
        shift = shift - mean * scale
        wide = lambda x: jnp.concatenate([x[t : t + 1] for t in range(tiles)], axis=1) * 0.5
        return wide(scale), wide(shift)

    def put_line(line, v, scale, shift, halves=(0, 1), shifted=True):
        a = half_silu(v, scale, shift)
        taps = column_shifts(a) if shifted else (None, a.astype(BF16), None)
        for j, x in enumerate(taps):
            if x is not None:
                for n, half in enumerate(halves):
                    act[half, j, line] = x[:, HALF * n : HALF * n + HALF]

    def halo_lines(copies, above, below, scale, shift, halves=(0, 1), shifted=True):
        taps = range(3) if shifted else (1,)
        for has, copy, ref, line in (
            (has_above, copies[0], above, 0),
            (has_below, copies[1], below, R + 1),
        ):
            @pl.when(has)
            def _():
                copy.wait_recv()
                put_line(line, ref[...].astype(F32), scale, shift, halves, shifted)

            @pl.when(jnp.logical_not(has))
            def _():
                for half in halves:
                    for j in taps:
                        act[half, j, line] = jnp.zeros((W, HALF), BF16)

    def start_down(copies):
        @pl.when(has_below)
        def _():
            copies[0].start()

    def start_up(copies):
        @pl.when(has_above)
        def _():
            copies[1].start()

    def end_sends(copies):
        @pl.when(has_below)
        def _():
            copies[0].wait_send()

        @pl.when(has_above)
        def _():
            copies[1].wait_send()

    def conv(lhs_of, weight_of, width, finish_lines):
        def block(b, carry):
            s, q = carry
            lo = 2 * b
            hi = R - 2 - 2 * b
            acc = None
            for i in range(3):
                for j in range(3):
                    lhs = jnp.concatenate([lhs_of(j, lo + i), lhs_of(j, hi + i)], axis=0)
                    d = jnp.dot(lhs, weight_of(3 * i + j), preferred_element_type=F32)
                    acc = d if acc is None else acc + d
            return finish_lines(b, lo, hi, acc, s, q)

        zero = jnp.zeros((8, width), F32)
        return lax.fori_loop(0, 2, block, (zero, zero))

    def two_lines(half, j, line):
        return act[half, j, pl.ds(line, 2)].reshape(2 * W, HALF)

    c_vid.wait()
    begin(c_w1)

    def video_sums(r, carry):
        s, q = carry
        a, b = partial_sums(vid[r + 1].astype(F32))
        return s + a, q + b

    zero = jnp.zeros((8, C), F32)
    s, q = lax.fori_loop(0, R, video_sums, (zero, zero))

    later = sum(1 - lax.div(f + k, n_frames) for k in range(1, BACK + 1))
    lines = 2 + lax.div(rr + n_rows - 1, n_rows) - lax.div(rr + 1, n_rows)
    pl.semaphore_wait(barrier, n_rows - 1 + later * lines)

    copies = send_stats(0, s, q)
    vh = halo(vid.at[R], vid.at[1], vid.at[0], vid.at[R + 1], vh_sem)
    start_down(vh)
    start_up(vh)
    c_w2.start()
    begin(c_t)

    finish([c_tiw])
    wbf[...] = jnp.zeros(wbf.shape, F32)
    for t in range(3):
        for j in range(3):
            for i in range(3):
                piece = tiwv[t, i, j].astype(F32)
                for n in range(R + 4):
                    top = 64 * j + 4 * (n + 1 + i)
                    wbf[top : top + 4, T * n : T * n + T] = piece
        for n in range(3):
            wb[n, 256 * t : 256 * t + 256] = wbf[:, 512 * n : 512 * n + 512].astype(BF16)

    finish(c_par + c_cb)
    scale, shift = norm_terms(0, copies, params[0], params[1])

    def video_line(r, _):
        put_line(r + 1, vid[r + 1].astype(F32), scale, shift)
        return 0

    lax.fori_loop(0, R, video_line, 0)
    halo_lines(vh, vid.at[0], vid.at[R + 1], scale, shift)
    finish(c_w1)

    hh = [halo(hsend.at[i, 1], hsend.at[i, 0], hrecv.at[i, 0], hrecv.at[i, 1], hh_sem.at[i]) for i in range(2)]
    h_copies = []
    for half in range(2):

        def h_lines(b, lo, hi, acc, s, q):
            v = acc + cbias[0, :, HALF * half : HALF * half + HALF]
            h[half, pl.ds(lo, 2)] = v[: 2 * W].reshape(2, W, HALF)
            h[half, pl.ds(hi, 2)] = v[2 * W :].reshape(2, W, HALF)

            @pl.when(b == 0)
            def _():
                hsend[half, 0] = v[:W].astype(BF16)
                hsend[half, 1] = v[3 * W :].astype(BF16)
                start_down(hh[half])
                start_up(hh[half])

            a, c = partial_sums(v)
            return s + a, q + c

        s, q = conv(
            lambda j, line: jnp.concatenate([two_lines(0, j, line), two_lines(1, j, line)], axis=1),
            lambda tap: w1[half, tap],
            HALF,
            h_lines,
        )
        h_copies.append(send_stats(1 + half, s, q))

    def h_norm(half):
        scale, shift = norm_terms(
            1 + half, h_copies[half], params[2, 2 * half : 2 * half + 2], params[3, 2 * half : 2 * half + 2]
        )

        def h_line(r, _):
            put_line(r + 1, h[half, r], scale, shift, (half,))
            return 0

        lax.fori_loop(0, R, h_line, 0)
        halo_lines(hh[half], hrecv.at[half, 0], hrecv.at[half, 1], scale, shift, (half,))

    h_norm(0)
    c_w2.wait()

    yh = halo(ysend.at[1], ysend.at[0], yrecv.at[0], yrecv.at[1], yh_sem)

    def y_part(b, lo, hi, acc, s, q):
        res = jnp.concatenate(
            [vid[pl.ds(lo + 1, 2)].reshape(2 * W, C), vid[pl.ds(hi + 1, 2)].reshape(2 * W, C)],
            axis=0,
        )
        v = res.astype(F32) + (acc + cbias[1])
        yp[pl.ds(lo, 2)] = v[: 2 * W].reshape(2, W, C)
        yp[pl.ds(hi, 2)] = v[2 * W :].reshape(2, W, C)
        return s, q

    def y_lines(b, lo, hi, acc, s, q):
        part = jnp.concatenate(
            [yp[pl.ds(lo, 2)].reshape(2 * W, C), yp[pl.ds(hi, 2)].reshape(2 * W, C)], axis=0
        )
        v = part + acc
        for half in range(2):
            x = v[:, HALF * half : HALF * half + HALF]
            h[half, pl.ds(lo, 2)] = x[: 2 * W].reshape(2, W, HALF)
            h[half, pl.ds(hi, 2)] = x[2 * W :].reshape(2, W, HALF)

        @pl.when(b == 0)
        def _():
            ysend[0] = v[:W].astype(BF16)
            ysend[1] = v[3 * W :].astype(BF16)
            start_down(yh)
            start_up(yh)

        a, c = partial_sums(v)
        return s + a, q + c

    conv(lambda j, line: two_lines(0, j, line), lambda tap: w2[tap, 0:HALF], C, y_part)

    h_norm(1)

    s, q = conv(lambda j, line: two_lines(1, j, line), lambda tap: w2[tap, HALF:C], C, y_lines)

    copies = send_stats(3, s, q)
    finish([c_ow] + c_q + c_tp)
    nt = (((1,), (1,)), ((), ()))
    pt[...] = jnp.zeros(pt.shape, F32)
    for t in range(3):
        for dst in (w1r, w2r):
            dst[t, 3, :, 0:T] = jnp.zeros((3 * T, T), BF16)
            dst[t, 0, :, T : 2 * T] = jnp.zeros((3 * T, T), BF16)
    row = lax.broadcasted_iota(jnp.int32, (4 * R, 8 * R), 0)
    col = lax.broadcasted_iota(jnp.int32, (4 * R, 8 * R), 1)
    quant = jnp.zeros((4 * R, 8 * R), F32)
    for m in range(8):
        for c in range(4):
            hit = (row % 4 == c) & (col % 8 == m) & (row // 4 == col // 8)
            quant = quant + jnp.where(hit, qwv[c : c + 1, m : m + 1], 0.0)
    row8 = lax.broadcasted_iota(jnp.int32, (8 * R, 1), 0)
    row4 = lax.broadcasted_iota(jnp.int32, (4 * R, 1), 0)
    head_bias = jnp.zeros((8 * R, 1), F32)
    for m in range(8):
        head_bias = head_bias + jnp.where(row8 % 8 == m, obv[0:1, m : m + 1], 0.0)
    quant_bias = jnp.zeros((4 * R, 1), F32)
    for c in range(4):
        quant_bias = quant_bias + jnp.where(row4 % 4 == c, qbv[0:1, c : c + 1], 0.0)

    scale, shift = norm_terms(3, copies, params[4], params[5])

    def y_line(r, _):
        v = jnp.concatenate([h[0, r], h[1, r]], axis=1)
        put_line(r + 1, v, scale, shift, shifted=False)
        return 0

    lax.fori_loop(0, R, y_line, 0)
    halo_lines(yh, yrecv.at[0], yrecv.at[1], scale, shift, shifted=False)

    for r in range(R + 2):
        line = jnp.concatenate([act[0, 1, r], act[1, 1, r]], axis=1)
        pt[r, :, 0:W] = lax.dot_general(wht[...], line, nt, preferred_element_type=F32)
    for r in range(R):
        sums = []
        for j in range(3):
            x = None
            for i in range(3):
                top = 8 * (3 * i + j)
                p = pt[r + i, top : top + 8, :]
                x = p if x is None else x + p
            sums.append(x)
        mom[8 * r : 8 * r + 8] = (
            sums[1] + pltpu.roll(sums[0], 1, 1) + pltpu.roll(sums[2], LANES - 1, 1)
        )
    means = (
        jnp.dot(quant, mom[...] + head_bias, precision=lax.Precision.HIGHEST, preferred_element_type=F32)
        + quant_bias
    )
    inside = lax.broadcasted_iota(jnp.int32, means.shape, 1) < W
    latent = jnp.where(inside, LATENT_SCALE * means, 0.0).astype(BF16)
    latsend[...] = latent
    lx[0, 16:48] = latent

    def lat_copy(k, d):
        src = {0: latsend, 1: latsend.at[pl.ds(16, 16)], -1: latsend.at[pl.ds(0, 16)]}[d]
        at = {0: pl.ds(16, 32), 1: pl.ds(0, 16), -1: pl.ds(48, 16)}[d]
        return pltpu.make_async_remote_copy(
            src_ref=src, dst_ref=lx.at[k, at],
            send_sem=lat_send.at[k, d + 1], recv_sem=lat_recv.at[k, d + 1],
            device_id={"frames": f + k, "rows": rr + d}, device_id_type=MESH,
        )

    for k, d in lat_targets():
        @pl.when(sends_to(k, d))
        def _():
            lat_copy(k, d).start()

    line16 = lax.broadcasted_iota(jnp.int32, (64, LANES), 0) // 16
    column = lax.broadcasted_iota(jnp.int32, (W, 128), 0)
    lowest = jnp.where(has_above, 0, 1)
    highest = jnp.where(has_below, 4, 3)

    def take_latent(k, dirs=(-1, 0, 1)):
        for d in dirs:
            @pl.when(gets_from(k, d))
            def _():
                lat_copy(k, d).wait_recv()
        keep = (line16 >= jnp.where(f >= k, lowest, 4)) & (line16 < highest)
        x = jnp.where(keep, lx[k].astype(F32), 0.0)
        x = jnp.transpose(jnp.concatenate([x, jnp.zeros((64, LANES), F32)], axis=0))[:W]
        left = jnp.where(column == 0, 0.0, pltpu.roll(x, 1, 0))
        right = jnp.where(column == W - 1, 0.0, pltpu.roll(x, W - 1, 0))
        ltt[k, :, 0:128] = (left + pltpu.roll(x, 64, 1)).astype(BF16)
        ltt[k, :, 128:256] = right.astype(BF16)

    def send_time_stats(e, s, q):
        tstbuf[e, rr, 0:1] = jnp.sum(s, axis=0, keepdims=True)
        tstbuf[e, rr, 1:2] = jnp.sum(q, axis=0, keepdims=True)
        begin(stat_copies(tstbuf.at[e], 4 + e))

    def time_terms(e, gain, shift):
        finish(stat_copies(tstbuf.at[e], 4 + e))
        total = tstbuf[e, 0]
        for r in range(1, n_rows):
            total = total + tstbuf[e, r]
        total = lane_group_sum(total, T // GROUPS) * (1.0 / (n_rows * R * W * (T // GROUPS)))
        mean = total[0:1]
        var = jnp.maximum(total[1:2] - mean * mean, 0.0)
        scale = lax.rsqrt(var + EPS) * gain
        return 0.5 * scale, 0.5 * (shift - mean * scale)

    def time_lines(src, dst, g, n_lines, margin, terms):
        scale, shift = terms

        def lines(m, _):
            for n in (2 * m, 2 * m + 1):
                at = R * rr + n - margin
                ok = jnp.logical_and(jnp.logical_and(at >= 0, at < n_rows * R), f >= g)
                a = jnp.where(ok, half_silu(src[g, n], scale, shift), 0.0)
                for j, x in enumerate(column_shifts(a)):
                    dst[g, n, :, T * j : T * j + T] = x
            return 0

        lax.fori_loop(0, n_lines // 2, lines, 0)

    def pair_lines(src, g, i, pairs):
        return jnp.concatenate([src[g, 2 * p + i] for p in range(pairs)], axis=0)

    take_latent(0, (-1, 1))
    take_latent(1)

    def t0_frame(g, _):
        take_latent(g + 2)
        lhs = jnp.concatenate([ltt[g + 2], ltt[g + 1], ltt[g]], axis=1)
        s = jnp.zeros((8, T), F32)
        q = jnp.zeros((8, T), F32)
        for n in range(3):
            acc = jnp.dot(lhs, wb[n], preferred_element_type=F32)
            for m in range(4):
                v = acc[:, T * m : T * m + T] + tparams[0]
                t0s[g, 4 * n + m] = v
                if 2 <= 4 * n + m < R + 2:
                    a, c = partial_sums(v)
                    s += a
                    q += c
        send_time_stats(g, s, q)
        return 0

    lax.fori_loop(0, 5, t0_frame, 0)

    finish(c_t)

    def b1_frame(g):
        time_lines(t0s, b1, g, R + 4, 2, time_terms(g, tparams[1], tparams[2]))

    def b1_first(g, _):
        b1_frame(g)
        return 0

    lax.fori_loop(0, 2, b1_first, 0)

    def t1_frame(g, _):
        b1_frame(g + 2)
        pairs = R // 2 + 1
        lhs = jnp.concatenate(
            [pair_lines(b1, g + 2 - t, i, pairs) for t in range(3) for i in range(4)], axis=1
        )
        acc = jnp.dot(lhs, w1r[...].reshape(12 * 3 * T, 2 * T), preferred_element_type=F32)
        s = jnp.zeros((8, T), F32)
        q = jnp.zeros((8, T), F32)
        for p in range(pairs):
            for half in range(2):
                v = acc[W * p : W * p + W, T * half : T * half + T]
                t1s[g, 2 * p + half] = v
                if 1 <= 2 * p + half < R + 1:
                    a, c = partial_sums(v)
                    s += a
                    q += c
        send_time_stats(5 + g, s, q)
        return 0

    lax.fori_loop(0, 3, t1_frame, 0)

    for p in range(R // 2):
        for half in range(2):
            facc[W * p : W * p + W, T * half : T * half + T] = t0s[0, 2 * p + half + 2] + tparams[5]

    def feature_frame(g, _):
        time_lines(t1s, b2, g, R + 2, 1, time_terms(5 + g, tparams[3], tparams[4]))
        lhs = jnp.concatenate([pair_lines(b2, g, i, R // 2) for i in range(4)], axis=1)
        facc[...] += jnp.dot(
            lhs, w2r[2 - g].reshape(4 * 3 * T, 2 * T), preferred_element_type=F32
        )
        return 0

    lax.fori_loop(0, 3, feature_frame, 0)

    for p in range(R // 2):
        for half in range(2):
            out[2 * p + half] = facc[W * p : W * p + W, T * half : T * half + T].astype(BF16)
    end_sends(vh)
    end_sends(hh[0])
    end_sends(hh[1])
    end_sends(yh)
    for k, d in lat_targets():
        @pl.when(sends_to(k, d))
        def _():
            lat_copy(k, d).wait_send()


def body(
    video, norm1_gain, norm1_shift, conv1_weight, conv1_bias, norm2_gain, norm2_shift,
    conv2_weight, conv2_bias, out_gain, out_shift, out_weight, out_bias, quant_weight,
    quant_bias, time_in_weight, time_in_bias, tnorm1_gain, tnorm1_shift, time1_weight,
    tnorm2_gain, tnorm2_shift, time2_weight, time2_bias, *, n_frames, n_rows,
):
    tile = lambda a: a.reshape(4, 128)
    flat = lambda a: a.reshape(1, -1)
    args = (
        video.reshape(R, W, C),
        tile(norm1_gain), tile(norm1_shift), conv1_weight.reshape(9, C, C), flat(conv1_bias),
        tile(norm2_gain), tile(norm2_shift), conv2_weight.reshape(9, C, C), flat(conv2_bias),
        tile(out_gain), tile(out_shift), out_weight.transpose(0, 1, 3, 2).reshape(72, C), flat(out_bias),
        quant_weight.T, flat(quant_bias), time_in_weight, flat(time_in_bias),
        flat(tnorm1_gain), flat(tnorm1_shift), time1_weight.reshape(3, 3, 3 * T, T),
        flat(tnorm2_gain), flat(tnorm2_shift), time2_weight.reshape(3, 3, 3 * T, T),
        flat(time2_bias),
    )
    vmem = lambda *shape, dtype=BF16: pltpu.VMEM(shape, dtype)
    dma = pltpu.SemaphoreType.DMA
    result = pl.pallas_call(
        functools.partial(kernel, n_frames, n_rows),
        out_shape=jax.ShapeDtypeStruct((R, W, T), BF16),
        in_specs=[pl.BlockSpec(memory_space=pl.ANY)] * len(args),
        out_specs=pl.BlockSpec(memory_space=pltpu.VMEM),
        scratch_shapes=[
            vmem(R + 2, W, C),
            vmem(2, 9, C, HALF),
            vmem(9, C, C),
            vmem(2, 3, R + 2, W, HALF),
            vmem(2, R, W, HALF, dtype=F32),
            vmem(R, W, C, dtype=F32),
            vmem(2, 2, W, HALF),
            vmem(2, 2, W, HALF),
            vmem(2, W, C),
            vmem(2, W, C),
            vmem(6, 4, 128, dtype=F32),
            vmem(2, 1, C, dtype=F32),
            vmem(6, 1, T, dtype=F32),
            vmem(1, 8, dtype=F32),
            vmem(4, 8, dtype=F32),
            vmem(1, 4, dtype=F32),
            vmem(3, 3, 3, 4, T),
            vmem(72, C),
            vmem(R + 2, 72, LANES, dtype=F32),
            vmem(8 * R, LANES, dtype=F32),
            vmem(256, 12 * T, dtype=F32),
            vmem(3, 768, 4 * T),
            vmem(3, 4, 3 * T, 2 * T),
            vmem(3, 4, 3 * T, 2 * T),
            vmem(4, n_rows, 8, 128, dtype=F32),
            vmem(8, n_rows, 8, 128, dtype=F32),
            vmem(4 * R, LANES),
            vmem(BACK + 1, 64, LANES),
            vmem(BACK + 1, W, 256),
            vmem(5, R + 4, W, T, dtype=F32),
            vmem(5, R + 4, W, 3 * T),
            vmem(3, R + 2, W, T, dtype=F32),
            vmem(3, R + 2, W, 3 * T),
            vmem(R // 2 * W, 2 * T, dtype=F32),
            dma((28,)),
            dma((4,)),
            dma((2, 4)),
            dma((4,)),
            dma((12, 2, n_rows - 1)),
            dma((BACK + 1, 3)),
            dma((BACK + 1, 3)),
        ],
        compiler_params=pltpu.CompilerParams(
            collective_id=0, has_side_effects=True, vmem_limit_bytes=60 * 1024 * 1024
        ),
        name="encoder_window",
    )(*args)
    return result[None]


def solution(mesh):
    step = functools.partial(body, n_frames=mesh.shape["frames"], n_rows=mesh.shape["rows"])
    return jax.shard_map(
        step,
        mesh=mesh,
        in_specs=(P("frames", "rows", None, None),) + (P(),) * 23,
        out_specs=P("frames", "rows", None, None),
        check_vma=False,
    )
```

```python
import functools

import jax
import jax.numpy as jnp
from jax import lax
from jax.experimental import pallas as pl
from jax.experimental.pallas import tpu as pltpu
from jax.sharding import PartitionSpec as P

GROUPS = 32
EPS = 1e-06
LATENT_SCALE = 0.13025

R = 8
W = 160
C = 512
T = 128
HALF = C // 2
LANES = 256
SLOTS = 80
BACK = 6

MESH = pl.DeviceIdType.MESH
F32 = jnp.float32
BF16 = jnp.bfloat16


def lane_group_sum(x, size):
    lane = lax.broadcasted_iota(jnp.int32, x.shape, 1)
    step = 1
    while step < size:
        up = pltpu.roll(x, step, 1)
        down = pltpu.roll(x, 128 - step, 1)
        x = x + jnp.where((lane // step) % 2 == 1, up, down)
        step *= 2
    return x


def column_shifts(a):
    row = lax.broadcasted_iota(jnp.int32, (8, a.shape[1]), 0)
    left = pltpu.roll(a, 1, 0)
    left = jnp.concatenate([jnp.where(row == 0, 0.0, left[:8]), left[8:]], axis=0)
    right = pltpu.roll(a, W - 1, 0)
    right = jnp.concatenate([right[: W - 8], jnp.where(row == 7, 0.0, right[W - 8 :])], axis=0)
    return left.astype(BF16), a.astype(BF16), right.astype(BF16)


def half_silu(v, scale, shift):
    w = v * scale + shift
    return w * jnp.tanh(w) + w


def packed_row(line):
    if line < 0:
        return 5 * (line + 3)
    if line < R:
        return 16 + 5 * line
    return 64 + 5 * (line - R)


def partial_sums(v):
    g = v.reshape(-1, 8, v.shape[-1])
    return jnp.sum(g, axis=0), jnp.sum(g * g, axis=0)


def kernel(
    n_frames,
    n_rows,
    video, g1, s1, cw1, cb1, g2, s2, cw2, cb2, g3, s3, ow, ob, qw, qb,
    tiw, tib, tg1, ts1, tw1, tg2, ts2, tw2, tb2,
    out,
    vid, w1, w2, act, h, yp, hsend, hrecv, ysend, yrecv,
    params, cbias, tparams, obv, qwv, qbv, tiwv,
    wht, pt, mom, wbf, wb, w1r, w2r,
    stbuf, tstbuf, latsend, lx, ltt, t0s, b1, t1s, b2, facc,
    in_sem, vh_sem, hh_sem, yh_sem, st_sem, lat_send, lat_recv,
):
    f = lax.axis_index("frames")
    rr = lax.axis_index("rows")

    def local(src, dst, k):
        return pltpu.make_async_copy(src, dst, in_sem.at[k])

    c_vid = local(video, vid.at[pl.ds(1, R)], 0)
    c_w1 = [local(cw1.at[:, :, pl.ds(HALF * i, HALF)], w1.at[i], (1, 26)[i]) for i in range(2)]
    c_w2 = local(cw2, w2, 2)
    c_par = [local(a, params.at[i], 3 + i) for i, a in enumerate((g1, s1, g2, s2, g3, s3))]
    c_cb = [
        local(a.at[:, pl.ds(HALF * n, HALF)], cbias.at[i, n], (9, 27)[n] + i)
        for i, a in enumerate((cb1, cb2))
        for n in range(2)
    ]
    c_tp = [local(a, tparams.at[i], 11 + i) for i, a in enumerate((tib, tg1, ts1, tg2, ts2, tb2))]
    c_ow = local(ow, wht, 17)
    c_q = [local(ob, obv, 18), local(qw, qwv, 19), local(qb, qbv, 20)]
    c_tiw = local(tiw, tiwv, 21)
    c_t = []
    for i, (src, dst) in enumerate(((tw1, w1r), (tw2, w2r))):
        for p in range(2):
            c_t.append(local(src, dst.at[:, pl.ds(p, 3), :, pl.ds(T * p, T)], 22 + 2 * i + p))

    def begin(copies):
        for c in copies:
            c.start()

    def finish(copies):
        for c in copies:
            c.wait()

    def lat_targets():
        for k in range(BACK + 1):
            for d in (-1, 0, 1):
                if k or d:
                    yield k, d

    def sends_to(k, d):
        ok = f + k < n_frames
        if d == -1:
            ok = jnp.logical_and(ok, rr > 0)
        if d == 1:
            ok = jnp.logical_and(ok, rr < n_rows - 1)
        return ok

    def gets_from(k, d):
        ok = f >= k
        if d == -1:
            ok = jnp.logical_and(ok, rr < n_rows - 1)
        if d == 1:
            ok = jnp.logical_and(ok, rr > 0)
        return ok

    c_vid.start()
    stbuf[...] = jnp.zeros(stbuf.shape, F32)
    tstbuf[...] = jnp.zeros(tstbuf.shape, F32)
    barrier = pltpu.get_barrier_semaphore()
    for d in range(1, n_rows):
        pl.semaphore_signal(
            barrier, inc=1, device_id={"frames": f, "rows": lax.rem(rr + d, n_rows)},
            device_id_type=MESH,
        )
    for k, d in lat_targets():
        if k:
            @pl.when(gets_from(k, d))
            def _():
                pl.semaphore_signal(
                    barrier, inc=1, device_id={"frames": f - k, "rows": rr - d}, device_id_type=MESH
                )

    begin(c_par + c_cb + c_tp + [c_ow] + c_q + [c_tiw])

    def halo(src_last, src_first, dst_above, dst_below, sem):
        down = pltpu.make_async_remote_copy(
            src_ref=src_last, dst_ref=dst_above, send_sem=sem.at[0], recv_sem=sem.at[1],
            device_id={"frames": f, "rows": rr + 1}, device_id_type=MESH,
        )
        up = pltpu.make_async_remote_copy(
            src_ref=src_first, dst_ref=dst_below, send_sem=sem.at[2], recv_sem=sem.at[3],
            device_id={"frames": f, "rows": rr - 1}, device_id_type=MESH,
        )
        return down, up

    has_above = rr > 0
    has_below = rr < n_rows - 1

    def stat_copies(buf, e):
        return [
            pltpu.make_async_remote_copy(
                src_ref=buf.at[rr], dst_ref=buf.at[rr],
                send_sem=st_sem.at[e, 0, d - 1], recv_sem=st_sem.at[e, 1, d - 1],
                device_id={"frames": f, "rows": lax.rem(rr + d, n_rows)}, device_id_type=MESH,
            )
            for d in range(1, n_rows)
        ]

    def send_stats(e, s, q):
        s = jnp.sum(s, axis=0, keepdims=True)
        q = jnp.sum(q, axis=0, keepdims=True)
        tiles = s.shape[1] // 128
        for t in range(tiles):
            stbuf[e, rr, t : t + 1, :] = s[:, 128 * t : 128 * t + 128]
            stbuf[e, rr, tiles + t : tiles + t + 1, :] = q[:, 128 * t : 128 * t + 128]
        copies = stat_copies(stbuf.at[e], e)
        begin(copies)
        return copies

    def norm_terms(e, copies, gain, shift):
        finish(copies)
        tiles = gain.shape[0]
        total = stbuf[e, 0]
        for r in range(1, n_rows):
            total = total + stbuf[e, r]
        total = lane_group_sum(total, C // GROUPS) * (1.0 / (n_rows * R * W * (C // GROUPS)))
        mean = total[0:tiles]
        var = jnp.maximum(total[tiles : 2 * tiles] - mean * mean, 0.0)
        scale = lax.rsqrt(var + EPS) * gain
        shift = shift - mean * scale
        wide = lambda x: jnp.concatenate([x[t : t + 1] for t in range(tiles)], axis=1) * 0.5
        return wide(scale), wide(shift)

    def put_line(line, v, scale, shift, halves=(0, 1), shifted=True):
        a = half_silu(v, scale, shift)
        taps = column_shifts(a) if shifted else (None, a.astype(BF16), None)
        for j, x in enumerate(taps):
            if x is not None:
                for n, half in enumerate(halves):
                    act[half, j, line] = x[:, HALF * n : HALF * n + HALF]

    def halo_lines(copies, above, below, scale, shift, halves=(0, 1), shifted=True):
        taps = range(3) if shifted else (1,)
        for has, copy, ref, line in (
            (has_above, copies[0], above, 0),
            (has_below, copies[1], below, R + 1),
        ):
            @pl.when(has)
            def _():
                copy.wait_recv()
                put_line(line, ref[...].astype(F32), scale, shift, halves, shifted)

            @pl.when(jnp.logical_not(has))
            def _():
                for half in halves:
                    for j in taps:
                        act[half, j, line] = jnp.zeros((W, HALF), BF16)

    def start_down(copies):
        @pl.when(has_below)
        def _():
            copies[0].start()

    def start_up(copies):
        @pl.when(has_above)
        def _():
            copies[1].start()

    def end_sends(copies):
        @pl.when(has_below)
        def _():
            copies[0].wait_send()

        @pl.when(has_above)
        def _():
            copies[1].wait_send()

    def conv(lhs_of, weight_of, width, finish_lines):
        def block(b, carry):
            s, q = carry
            lo = 2 * b
            hi = R - 2 - 2 * b
            acc = None
            for i in range(3):
                for j in range(3):
                    lhs = jnp.concatenate([lhs_of(j, lo + i), lhs_of(j, hi + i)], axis=0)
                    d = jnp.dot(lhs, weight_of(3 * i + j), preferred_element_type=F32)
                    acc = d if acc is None else acc + d
            return finish_lines(b, lo, hi, acc, s, q)

        zero = jnp.zeros((8, width), F32)
        return lax.fori_loop(0, 2, block, (zero, zero))

    def two_lines(half, j, line):
        return act[half, j, pl.ds(line, 2)].reshape(2 * W, HALF)

    c_vid.wait()
    begin(c_w1)

    def video_sums(r, carry):
        s, q = carry
        a, b = partial_sums(vid[r + 1].astype(F32))
        return s + a, q + b

    zero = jnp.zeros((8, C), F32)
    s, q = lax.fori_loop(0, R, video_sums, (zero, zero))

    later = sum(1 - lax.div(f + k, n_frames) for k in range(1, BACK + 1))
    lines = 2 + lax.div(rr + n_rows - 1, n_rows) - lax.div(rr + 1, n_rows)
    pl.semaphore_wait(barrier, n_rows - 1 + later * lines)

    copies = send_stats(0, s, q)
    vh = halo(vid.at[R], vid.at[1], vid.at[0], vid.at[R + 1], vh_sem)
    start_down(vh)
    start_up(vh)
    c_w2.start()
    begin(c_t)

    finish([c_tiw])
    wbf[...] = jnp.zeros(wbf.shape, F32)
    for t in range(3):
        for j in range(3):
            for i in range(3):
                piece = tiwv[t, i, j].astype(F32)
                for n in range(R + 4):
                    top = SLOTS * j + packed_row(n + i - 3)
                    wbf[top : top + 4, T * n : T * n + T] = piece
        for n in range(3):
            wb[n, 256 * t : 256 * t + 256] = wbf[:, 512 * n : 512 * n + 512].astype(BF16)

    finish(c_par + c_cb)
    scale, shift = norm_terms(0, copies, params[0], params[1])

    def video_line(r, _):
        put_line(r + 1, vid[r + 1].astype(F32), scale, shift)
        return 0

    lax.fori_loop(0, R, video_line, 0)
    halo_lines(vh, vid.at[0], vid.at[R + 1], scale, shift)
    finish(c_w1)

    hh = [halo(hsend.at[i, 1], hsend.at[i, 0], hrecv.at[i, 0], hrecv.at[i, 1], hh_sem.at[i]) for i in range(2)]

    def h_half(half, _):
        acc = None
        for i in range(3):
            for j in range(3):
                lhs = jnp.concatenate(
                    [act[n, j, i : i + R].reshape(R * W, HALF) for n in range(2)], axis=1
                )
                d = jnp.dot(lhs, w1[half, 3 * i + j], preferred_element_type=F32)
                acc = d if acc is None else acc + d
        v = acc + cbias[0, half]
        h[half] = v.reshape(R, W, HALF)
        hsend[half, 0] = v[:W].astype(BF16)
        hsend[half, 1] = v[R * W - W :].astype(BF16)
        copies = halo(
            hsend.at[half, 1], hsend.at[half, 0], hrecv.at[half, 0], hrecv.at[half, 1], hh_sem.at[half]
        )
        send_stats(1 + half, *partial_sums(v))
        start_down(copies)
        start_up(copies)
        return 0

    lax.fori_loop(0, 2, h_half, 0)

    def h_norm(half):
        scale, shift = norm_terms(
            1 + half, stat_copies(stbuf.at[1 + half], 1 + half), params[2, 2 * half : 2 * half + 2], params[3, 2 * half : 2 * half + 2]
        )

        def h_line(r, _):
            put_line(r + 1, h[half, r], scale, shift, (half,))
            return 0

        lax.fori_loop(0, R, h_line, 0)
        halo_lines(hh[half], hrecv.at[half, 0], hrecv.at[half, 1], scale, shift, (half,))

    h_norm(0)
    c_w2.wait()

    yh = halo(ysend.at[1], ysend.at[0], yrecv.at[0], yrecv.at[1], yh_sem)

    def y_part(b, lo, hi, acc, s, q):
        res = jnp.concatenate(
            [vid[pl.ds(lo + 1, 2)].reshape(2 * W, C), vid[pl.ds(hi + 1, 2)].reshape(2 * W, C)],
            axis=0,
        )
        v = res.astype(F32) + (acc + jnp.concatenate([cbias[1, 0], cbias[1, 1]], axis=1))
        yp[pl.ds(lo, 2)] = v[: 2 * W].reshape(2, W, C)
        yp[pl.ds(hi, 2)] = v[2 * W :].reshape(2, W, C)
        return s, q

    def y_lines(b, lo, hi, acc, s, q):
        part = jnp.concatenate(
            [yp[pl.ds(lo, 2)].reshape(2 * W, C), yp[pl.ds(hi, 2)].reshape(2 * W, C)], axis=0
        )
        v = part + acc
        for half in range(2):
            x = v[:, HALF * half : HALF * half + HALF]
            h[half, pl.ds(lo, 2)] = x[: 2 * W].reshape(2, W, HALF)
            h[half, pl.ds(hi, 2)] = x[2 * W :].reshape(2, W, HALF)

        @pl.when(b == 0)
        def _():
            ysend[0] = v[:W].astype(BF16)
            ysend[1] = v[3 * W :].astype(BF16)
            start_down(yh)
            start_up(yh)

        a, c = partial_sums(v)
        return s + a, q + c

    conv(lambda j, line: two_lines(0, j, line), lambda tap: w2[tap, 0:HALF], C, y_part)

    h_norm(1)

    s, q = conv(lambda j, line: two_lines(1, j, line), lambda tap: w2[tap, HALF:C], C, y_lines)

    copies = send_stats(3, s, q)
    finish([c_ow] + c_q + c_tp)
    nt = (((1,), (1,)), ((), ()))
    pt[...] = jnp.zeros(pt.shape, F32)
    for t in range(3):
        for dst in (w1r, w2r):
            dst[t, 3, :, 0:T] = jnp.zeros((3 * T, T), BF16)
            dst[t, 0, :, T : 2 * T] = jnp.zeros((3 * T, T), BF16)
    row = lax.broadcasted_iota(jnp.int32, (48, 8 * R), 0)
    col = lax.broadcasted_iota(jnp.int32, (48, 8 * R), 1)
    quant = jnp.zeros((48, 8 * R), F32)
    for m in range(8):
        for c in range(4):
            hit = (row % 5 == c) & (col % 8 == m) & (row // 5 == col // 8)
            quant = quant + jnp.where(hit, qwv[c : c + 1, m : m + 1], 0.0)
    row8 = lax.broadcasted_iota(jnp.int32, (8 * R, 1), 0)
    row5 = lax.broadcasted_iota(jnp.int32, (48, 1), 0)
    head_bias = jnp.zeros((8 * R, 1), F32)
    for m in range(8):
        head_bias = head_bias + jnp.where(row8 % 8 == m, obv[0:1, m : m + 1], 0.0)
    quant_bias = jnp.zeros((48, 1), F32)
    for c in range(4):
        quant_bias = quant_bias + jnp.where(row5 % 5 == c, qbv[0:1, c : c + 1], 0.0)

    scale, shift = norm_terms(3, copies, params[4], params[5])

    def y_line(r, _):
        v = jnp.concatenate([h[0, r], h[1, r]], axis=1)
        put_line(r + 1, v, scale, shift, shifted=False)
        return 0

    lax.fori_loop(0, R, y_line, 0)
    halo_lines(yh, yrecv.at[0], yrecv.at[1], scale, shift, shifted=False)

    for r in range(R + 2):
        line = jnp.concatenate([act[0, 1, r], act[1, 1, r]], axis=1)
        pt[r, :, 0:W] = lax.dot_general(wht[...], line, nt, preferred_element_type=F32)
    for r in range(R):
        sums = []
        for j in range(3):
            x = None
            for i in range(3):
                top = 8 * (3 * i + j)
                p = pt[r + i, top : top + 8, :]
                x = p if x is None else x + p
            sums.append(x)
        mom[8 * r : 8 * r + 8] = (
            sums[1] + pltpu.roll(sums[0], 1, 1) + pltpu.roll(sums[2], LANES - 1, 1)
        )
    means = (
        jnp.dot(quant, mom[...] + head_bias, precision=lax.Precision.HIGHEST, preferred_element_type=F32)
        + quant_bias
    )
    means = LATENT_SCALE * means
    row = lax.broadcasted_iota(jnp.int32, (48, 128), 0)
    lane = lax.broadcasted_iota(jnp.int32, (48, 128), 1)
    rest = jnp.where((lane < W - 128) & (row < 5 * R), means[:, 128:256], 0.0)
    packed = jnp.where(row % 5 < 4, means[:, 0:128], 0.0)
    for c in range(4):
        moved = pltpu.roll(jnp.where(row % 5 == c, rest, 0.0), 4 - c, 0)
        packed = packed + (pltpu.roll(moved, 32 * c, 1) if c else moved)
    packed = jnp.where(row < 5 * R, packed, 0.0)
    latsend[0:48] = packed.astype(BF16)
    latsend[48:64] = pltpu.roll(packed, 48 - 25, 0)[0:16].astype(BF16)
    lx[0, 16:64] = packed.astype(BF16)

    def lat_copy(k, d):
        src = {0: pl.ds(0, 48), 1: pl.ds(48, 16), -1: pl.ds(0, 16)}[d]
        at = {0: pl.ds(16, 48), 1: pl.ds(0, 16), -1: pl.ds(64, 16)}[d]
        return pltpu.make_async_remote_copy(
            src_ref=latsend.at[src], dst_ref=lx.at[k, at],
            send_sem=lat_send.at[k, d + 1], recv_sem=lat_recv.at[k, d + 1],
            device_id={"frames": f + k, "rows": rr + d}, device_id_type=MESH,
        )

    for k, d in lat_targets():
        @pl.when(sends_to(k, d))
        def _():
            lat_copy(k, d).start()

    slot = lax.broadcasted_iota(jnp.int32, (SLOTS, 128), 0)
    lowest = jnp.where(has_above, 0, 16)
    highest = jnp.where(has_below, SLOTS, 64)
    column = lax.broadcasted_iota(jnp.int32, (W, 128), 0)
    lane = lax.broadcasted_iota(jnp.int32, (W, 128), 1)
    lane32 = lax.broadcasted_iota(jnp.int32, (32, 128), 1)
    fifth = lane32 < 0
    for line in range(-3, R + 3):
        fifth = fifth | (lane32 == packed_row(line) + 4)

    def take_latent(k, dirs=(-1, 0, 1)):
        for d in dirs:
            @pl.when(gets_from(k, d))
            def _():
                lat_copy(k, d).wait_recv()
        keep = (slot >= jnp.where(f >= k, lowest, SLOTS)) & (slot < highest)
        x = jnp.where(keep, lx[k].astype(F32), 0.0)
        x = jnp.transpose(jnp.concatenate([x, jnp.zeros((128 - SLOTS, 128), F32)], axis=0))
        rest = jnp.zeros((32, 128), F32)
        for c in range(4):
            rest = rest + pltpu.roll(jnp.where(fifth, x[32 * c : 32 * c + 32], 0.0), 128 + c - 4, 1)
        x = jnp.concatenate([x, rest], axis=0)
        left = jnp.where(column == 0, 0.0, pltpu.roll(x, 1, 0))
        right = jnp.where(column == W - 1, 0.0, pltpu.roll(x, W - 1, 0))
        centre = pltpu.roll(x, SLOTS, 1)
        ltt[k, :, 0:128] = jnp.where(lane < SLOTS, left, centre).astype(BF16)
        ltt[k, :, 128:256] = jnp.where(lane < 2 * SLOTS - 128, centre, pltpu.roll(right, 2 * SLOTS - 128, 1)).astype(BF16)

    def send_time_stats(e, s, q):
        tstbuf[e, rr, 0:1] = jnp.sum(s, axis=0, keepdims=True)
        tstbuf[e, rr, 1:2] = jnp.sum(q, axis=0, keepdims=True)
        begin(stat_copies(tstbuf.at[e], 4 + e))

    def time_terms(e, gain, shift):
        finish(stat_copies(tstbuf.at[e], 4 + e))
        total = tstbuf[e, 0]
        for r in range(1, n_rows):
            total = total + tstbuf[e, r]
        total = lane_group_sum(total, T // GROUPS) * (1.0 / (n_rows * R * W * (T // GROUPS)))
        mean = total[0:1]
        var = jnp.maximum(total[1:2] - mean * mean, 0.0)
        scale = lax.rsqrt(var + EPS) * gain
        return 0.5 * scale, 0.5 * (shift - mean * scale)

    def time_lines(src, dst, g, n_lines, margin, terms):
        scale, shift = terms

        def lines(m, _):
            for n in (2 * m, 2 * m + 1):
                at = R * rr + n - margin
                ok = jnp.logical_and(jnp.logical_and(at >= 0, at < n_rows * R), f >= g)
                a = half_silu(src[g, n], jnp.where(ok, scale, 0.0), jnp.where(ok, shift, 0.0))
                for j, x in enumerate(column_shifts(a)):
                    dst[g, n, :, T * j : T * j + T] = x
            return 0

        lax.fori_loop(0, n_lines // 2, lines, 0)

    def pair_lines(src, g, i, pairs):
        return jnp.concatenate([src[g, 2 * p + i] for p in range(pairs)], axis=0)

    take_latent(0, (-1, 1))
    take_latent(1)

    def t0_frame(g, _):
        take_latent(g + 2)
        lhs = jnp.concatenate([ltt[g + 2], ltt[g + 1], ltt[g]], axis=1)
        s = jnp.zeros((8, T), F32)
        q = jnp.zeros((8, T), F32)
        for n in range(3):
            acc = jnp.dot(lhs, wb[n], preferred_element_type=F32)
            for m in range(4):
                v = acc[:, T * m : T * m + T] + tparams[0]
                t0s[g, 4 * n + m] = v
                if 2 <= 4 * n + m < R + 2:
                    a, c = partial_sums(v)
                    s += a
                    q += c
        send_time_stats(g, s, q)
        return 0

    lax.fori_loop(0, 5, t0_frame, 0)

    finish(c_t)

    def b1_frame(g):
        time_lines(t0s, b1, g, R + 4, 2, time_terms(g, tparams[1], tparams[2]))

    def b1_first(g, _):
        b1_frame(g)
        return 0

    lax.fori_loop(0, 2, b1_first, 0)

    def t1_frame(g, _):
        b1_frame(g + 2)
        pairs = R // 2 + 1
        lhs = jnp.concatenate(
            [pair_lines(b1, g + 2 - t, i, pairs) for t in range(3) for i in range(4)], axis=1
        )
        acc = jnp.dot(lhs, w1r[...].reshape(12 * 3 * T, 2 * T), preferred_element_type=F32)
        s = jnp.zeros((8, T), F32)
        q = jnp.zeros((8, T), F32)
        for p in range(pairs):
            for half in range(2):
                v = acc[W * p : W * p + W, T * half : T * half + T]
                t1s[g, 2 * p + half] = v
                if 1 <= 2 * p + half < R + 1:
                    a, c = partial_sums(v)
                    s += a
                    q += c
        send_time_stats(5 + g, s, q)
        return 0

    lax.fori_loop(0, 3, t1_frame, 0)

    for p in range(R // 2):
        for half in range(2):
            facc[W * p : W * p + W, T * half : T * half + T] = t0s[0, 2 * p + half + 2] + tparams[5]

    def feature_frame(g, _):
        time_lines(t1s, b2, g, R + 2, 1, time_terms(5 + g, tparams[3], tparams[4]))
        lhs = jnp.concatenate([pair_lines(b2, g, i, R // 2) for i in range(4)], axis=1)
        facc[...] += jnp.dot(
            lhs, w2r[2 - g].reshape(4 * 3 * T, 2 * T), preferred_element_type=F32
        )
        return 0

    lax.fori_loop(0, 3, feature_frame, 0)

    for p in range(R // 2):
        for half in range(2):
            out[2 * p + half] = facc[W * p : W * p + W, T * half : T * half + T].astype(BF16)
    end_sends(vh)
    end_sends(hh[0])
    end_sends(hh[1])
    end_sends(yh)
    for k, d in lat_targets():
        @pl.when(sends_to(k, d))
        def _():
            lat_copy(k, d).wait_send()


def body(
    video, norm1_gain, norm1_shift, conv1_weight, conv1_bias, norm2_gain, norm2_shift,
    conv2_weight, conv2_bias, out_gain, out_shift, out_weight, out_bias, quant_weight,
    quant_bias, time_in_weight, time_in_bias, tnorm1_gain, tnorm1_shift, time1_weight,
    tnorm2_gain, tnorm2_shift, time2_weight, time2_bias, *, n_frames, n_rows,
):
    tile = lambda a: a.reshape(4, 128)
    flat = lambda a: a.reshape(1, -1)
    args = (
        video.reshape(R, W, C),
        tile(norm1_gain), tile(norm1_shift), conv1_weight.reshape(9, C, C), flat(conv1_bias),
        tile(norm2_gain), tile(norm2_shift), conv2_weight.reshape(9, C, C), flat(conv2_bias),
        tile(out_gain), tile(out_shift), out_weight.transpose(0, 1, 3, 2).reshape(72, C), flat(out_bias),
        quant_weight.T, flat(quant_bias), time_in_weight, flat(time_in_bias),
        flat(tnorm1_gain), flat(tnorm1_shift), time1_weight.reshape(3, 3, 3 * T, T),
        flat(tnorm2_gain), flat(tnorm2_shift), time2_weight.reshape(3, 3, 3 * T, T),
        flat(time2_bias),
    )
    vmem = lambda *shape, dtype=BF16: pltpu.VMEM(shape, dtype)
    dma = pltpu.SemaphoreType.DMA
    result = pl.pallas_call(
        functools.partial(kernel, n_frames, n_rows),
        out_shape=pltpu.VMEM((R, W, T), BF16),
        in_specs=[pl.BlockSpec(memory_space=pl.ANY)] * len(args),
        out_specs=pl.BlockSpec(memory_space=pltpu.VMEM),
        scratch_shapes=[
            vmem(R + 2, W, C),
            vmem(2, 9, C, HALF),
            vmem(9, C, C),
            vmem(2, 3, R + 2, W, HALF),
            vmem(2, R, W, HALF, dtype=F32),
            vmem(R, W, C, dtype=F32),
            vmem(2, 2, W, HALF),
            vmem(2, 2, W, HALF),
            vmem(2, W, C),
            vmem(2, W, C),
            vmem(6, 4, 128, dtype=F32),
            vmem(2, 2, 1, HALF, dtype=F32),
            vmem(6, 1, T, dtype=F32),
            vmem(1, 8, dtype=F32),
            vmem(4, 8, dtype=F32),
            vmem(1, 4, dtype=F32),
            vmem(3, 3, 3, 4, T),
            vmem(72, C),
            vmem(R + 2, 72, LANES, dtype=F32),
            vmem(8 * R, LANES, dtype=F32),
            vmem(256, 12 * T, dtype=F32),
            vmem(3, 768, 4 * T),
            vmem(3, 4, 3 * T, 2 * T),
            vmem(3, 4, 3 * T, 2 * T),
            vmem(4, n_rows, 8, 128, dtype=F32),
            vmem(8, n_rows, 8, 128, dtype=F32),
            vmem(64, 128),
            vmem(BACK + 1, SLOTS, 128),
            vmem(BACK + 1, W, 256),
            vmem(5, R + 4, W, T, dtype=F32),
            vmem(5, R + 4, W, 3 * T),
            vmem(3, R + 2, W, T, dtype=F32),
            vmem(3, R + 2, W, 3 * T),
            vmem(R // 2 * W, 2 * T, dtype=F32),
            dma((29,)),
            dma((4,)),
            dma((2, 4)),
            dma((4,)),
            dma((12, 2, n_rows - 1)),
            dma((BACK + 1, 3)),
            dma((BACK + 1, 3)),
        ],
        compiler_params=pltpu.CompilerParams(
            collective_id=0, has_side_effects=True, vmem_limit_bytes=60 * 1024 * 1024
        ),
        name="encoder_window",
    )(*args)
    return result[None]


def solution(mesh):
    step = functools.partial(body, n_frames=mesh.shape["frames"], n_rows=mesh.shape["rows"])
    return jax.shard_map(
        step,
        mesh=mesh,
        in_specs=(P("frames", "rows", None, None),) + (P(),) * 23,
        out_specs=P("frames", "rows", None, None),
        check_vma=False,
    )
```

```python
import functools

import jax
import jax.numpy as jnp
from jax import lax
from jax.experimental import pallas as pl
from jax.experimental.pallas import tpu as pltpu
from jax.sharding import PartitionSpec as P

GROUPS = 32
EPS = 1e-06
LATENT_SCALE = 0.13025

R = 8
W = 160
C = 512
T = 128
HALF = C // 2
LANES = 256
SLOTS = 80
BACK = 6

MESH = pl.DeviceIdType.MESH
F32 = jnp.float32
BF16 = jnp.bfloat16


def lane_group_sum(x, size):
    lane = lax.broadcasted_iota(jnp.int32, x.shape, 1)
    step = 1
    while step < size:
        up = pltpu.roll(x, step, 1)
        down = pltpu.roll(x, 128 - step, 1)
        x = x + jnp.where((lane // step) % 2 == 1, up, down)
        step *= 2
    return x


def column_shifts(a):
    row = lax.broadcasted_iota(jnp.int32, (8, a.shape[1]), 0)
    left = pltpu.roll(a, 1, 0)
    left = jnp.concatenate([jnp.where(row == 0, 0.0, left[:8]), left[8:]], axis=0)
    right = pltpu.roll(a, W - 1, 0)
    right = jnp.concatenate([right[: W - 8], jnp.where(row == 7, 0.0, right[W - 8 :])], axis=0)
    return left.astype(BF16), a.astype(BF16), right.astype(BF16)


def half_silu(v, scale, shift):
    w = v * scale + shift
    return w * jnp.tanh(w) + w


def packed_row(line):
    if line < 0:
        return 5 * (line + 3)
    if line < R:
        return 16 + 5 * line
    return 64 + 5 * (line - R)


def partial_sums(v):
    g = v.reshape(-1, 8, v.shape[-1])
    return jnp.sum(g, axis=0), jnp.sum(g * g, axis=0)


def kernel(
    n_frames,
    n_rows,
    video, g1, s1, cw1, cb1, g2, s2, cw2, cb2, g3, s3, ow, ob, qw, qb,
    tiw, tib, tg1, ts1, tw1, tg2, ts2, tw2, tb2,
    out,
    vid, w1, w2, act, h, yp, hsend, hrecv, ysend, yrecv,
    params, cbias, tparams, obv, qwv, qbv, tiwv,
    wht, pt, mom, wbf, wb, w1r, w2r,
    stbuf, tstbuf, latsend, lx, ltt, t0s, b1, t1s, t1send, t1recv, b2, facc,
    in_sem, vh_sem, hh_sem, yh_sem, th_sem, st_sem, lat_send, lat_recv,
):
    f = lax.axis_index("frames")
    rr = lax.axis_index("rows")

    def local(src, dst, k):
        return pltpu.make_async_copy(src, dst, in_sem.at[k])

    c_vid = local(video, vid.at[pl.ds(1, R)], 0)
    c_w1 = [local(cw1.at[:, :, pl.ds(HALF * i, HALF)], w1.at[i], (1, 26)[i]) for i in range(2)]
    c_w2 = local(cw2, w2, 2)
    c_par = [local(a, params.at[i], 3 + i) for i, a in enumerate((g1, s1, g2, s2, g3, s3))]
    c_cb = [
        local(a.at[:, pl.ds(HALF * n, HALF)], cbias.at[i, n], (9, 27)[n] + i)
        for i, a in enumerate((cb1, cb2))
        for n in range(2)
    ]
    c_tp = [local(a, tparams.at[i], 11 + i) for i, a in enumerate((tib, tg1, ts1, tg2, ts2, tb2))]
    c_ow = local(ow, wht, 17)
    c_q = [local(ob, obv, 18), local(qw, qwv, 19), local(qb, qbv, 20)]
    c_tiw = local(tiw, tiwv, 21)
    c_t = []
    for i, (src, dst) in enumerate(((tw1, w1r), (tw2, w2r))):
        for p in range(2):
            c_t.append(local(src, dst.at[:, pl.ds(p, 3), :, pl.ds(T * p, T)], 22 + 2 * i + p))

    def begin(copies):
        for c in copies:
            c.start()

    def finish(copies):
        for c in copies:
            c.wait()

    def lat_targets():
        for k in range(BACK + 1):
            for d in (-1, 0, 1):
                if k or d:
                    yield k, d

    def sends_to(k, d):
        ok = f + k < n_frames
        if d == -1:
            ok = jnp.logical_and(ok, rr > 0)
        if d == 1:
            ok = jnp.logical_and(ok, rr < n_rows - 1)
        return ok

    def gets_from(k, d):
        ok = f >= k
        if d == -1:
            ok = jnp.logical_and(ok, rr < n_rows - 1)
        if d == 1:
            ok = jnp.logical_and(ok, rr > 0)
        return ok

    c_vid.start()
    stbuf[...] = jnp.zeros(stbuf.shape, F32)
    tstbuf[...] = jnp.zeros(tstbuf.shape, F32)
    barrier = pltpu.get_barrier_semaphore()
    for d in range(1, n_rows):
        pl.semaphore_signal(
            barrier, inc=1, device_id={"frames": f, "rows": lax.rem(rr + d, n_rows)},
            device_id_type=MESH,
        )
    for k, d in lat_targets():
        if k:
            @pl.when(gets_from(k, d))
            def _():
                pl.semaphore_signal(
                    barrier, inc=1, device_id={"frames": f - k, "rows": rr - d}, device_id_type=MESH
                )

    begin(c_par + c_cb + c_tp + [c_ow] + c_q + [c_tiw])

    def halo(src_last, src_first, dst_above, dst_below, sem):
        down = pltpu.make_async_remote_copy(
            src_ref=src_last, dst_ref=dst_above, send_sem=sem.at[0], recv_sem=sem.at[1],
            device_id={"frames": f, "rows": rr + 1}, device_id_type=MESH,
        )
        up = pltpu.make_async_remote_copy(
            src_ref=src_first, dst_ref=dst_below, send_sem=sem.at[2], recv_sem=sem.at[3],
            device_id={"frames": f, "rows": rr - 1}, device_id_type=MESH,
        )
        return down, up

    has_above = rr > 0
    has_below = rr < n_rows - 1

    def stat_copies(buf, e):
        return [
            pltpu.make_async_remote_copy(
                src_ref=buf.at[rr], dst_ref=buf.at[rr],
                send_sem=st_sem.at[e, 0, d - 1], recv_sem=st_sem.at[e, 1, d - 1],
                device_id={"frames": f, "rows": lax.rem(rr + d, n_rows)}, device_id_type=MESH,
            )
            for d in range(1, n_rows)
        ]

    def send_stats(e, s, q):
        s = jnp.sum(s, axis=0, keepdims=True)
        q = jnp.sum(q, axis=0, keepdims=True)
        tiles = s.shape[1] // 128
        for t in range(tiles):
            stbuf[e, rr, t : t + 1, :] = s[:, 128 * t : 128 * t + 128]
            stbuf[e, rr, tiles + t : tiles + t + 1, :] = q[:, 128 * t : 128 * t + 128]
        copies = stat_copies(stbuf.at[e], e)
        begin(copies)
        return copies

    def norm_terms(e, copies, gain, shift):
        finish(copies)
        tiles = gain.shape[0]
        total = stbuf[e, 0]
        for r in range(1, n_rows):
            total = total + stbuf[e, r]
        total = lane_group_sum(total, C // GROUPS) * (1.0 / (n_rows * R * W * (C // GROUPS)))
        mean = total[0:tiles]
        var = jnp.maximum(total[tiles : 2 * tiles] - mean * mean, 0.0)
        scale = lax.rsqrt(var + EPS) * gain
        shift = shift - mean * scale
        wide = lambda x: jnp.concatenate([x[t : t + 1] for t in range(tiles)], axis=1) * 0.5
        return wide(scale), wide(shift)

    def put_line(line, v, scale, shift, halves=(0, 1), shifted=True):
        a = half_silu(v, scale, shift)
        taps = column_shifts(a) if shifted else (None, a.astype(BF16), None)
        for j, x in enumerate(taps):
            if x is not None:
                for n, half in enumerate(halves):
                    act[half, j, line] = x[:, HALF * n : HALF * n + HALF]

    def halo_lines(copies, above, below, scale, shift, halves=(0, 1), shifted=True):
        taps = range(3) if shifted else (1,)
        for has, copy, ref, line in (
            (has_above, copies[0], above, 0),
            (has_below, copies[1], below, R + 1),
        ):
            @pl.when(has)
            def _():
                copy.wait_recv()
                put_line(line, ref[...].astype(F32), scale, shift, halves, shifted)

            @pl.when(jnp.logical_not(has))
            def _():
                for half in halves:
                    for j in taps:
                        act[half, j, line] = jnp.zeros((W, HALF), BF16)

    def start_down(copies):
        @pl.when(has_below)
        def _():
            copies[0].start()

    def start_up(copies):
        @pl.when(has_above)
        def _():
            copies[1].start()

    def end_sends(copies):
        @pl.when(has_below)
        def _():
            copies[0].wait_send()

        @pl.when(has_above)
        def _():
            copies[1].wait_send()

    def conv(lhs_of, weight_of, width, finish_lines):
        def block(b, carry):
            s, q = carry
            lo = 2 * b
            hi = R - 2 - 2 * b
            acc = None
            for i in range(3):
                for j in range(3):
                    lhs = jnp.concatenate([lhs_of(j, lo + i), lhs_of(j, hi + i)], axis=0)
                    d = jnp.dot(lhs, weight_of(3 * i + j), preferred_element_type=F32)
                    acc = d if acc is None else acc + d
            return finish_lines(b, lo, hi, acc, s, q)

        zero = jnp.zeros((8, width), F32)
        return lax.fori_loop(0, 2, block, (zero, zero))

    def two_lines(half, j, line):
        return act[half, j, pl.ds(line, 2)].reshape(2 * W, HALF)

    c_vid.wait()
    begin(c_w1)

    def video_sums(r, carry):
        s, q = carry
        a, b = partial_sums(vid[r + 1].astype(F32))
        return s + a, q + b

    zero = jnp.zeros((8, C), F32)
    s, q = lax.fori_loop(0, R, video_sums, (zero, zero))

    later = sum(1 - lax.div(f + k, n_frames) for k in range(1, BACK + 1))
    lines = 2 + lax.div(rr + n_rows - 1, n_rows) - lax.div(rr + 1, n_rows)
    pl.semaphore_wait(barrier, n_rows - 1 + later * lines)

    copies = send_stats(0, s, q)
    vh = halo(vid.at[R], vid.at[1], vid.at[0], vid.at[R + 1], vh_sem)
    start_down(vh)
    start_up(vh)
    c_w2.start()
    begin(c_t)

    finish([c_tiw])
    wbf[...] = jnp.zeros(wbf.shape, F32)
    for t in range(3):
        for j in range(3):
            for i in range(3):
                piece = tiwv[t, i, j].astype(F32)
                for n in range(R + 2):
                    top = SLOTS * j + packed_row(n + i - 2)
                    wbf[top : top + 4, T * n : T * n + T] = piece
        wb[256 * t : 256 * t + 256] = wbf[...].astype(BF16)

    finish(c_par + c_cb)
    scale, shift = norm_terms(0, copies, params[0], params[1])

    def video_line(r, _):
        put_line(r + 1, vid[r + 1].astype(F32), scale, shift)
        return 0

    lax.fori_loop(0, R, video_line, 0)
    halo_lines(vh, vid.at[0], vid.at[R + 1], scale, shift)
    finish(c_w1)

    hh = [halo(hsend.at[i, 1], hsend.at[i, 0], hrecv.at[i, 0], hrecv.at[i, 1], hh_sem.at[i]) for i in range(2)]

    def h_half(half, _):
        acc = None
        for i in range(3):
            for j in range(3):
                lhs = jnp.concatenate(
                    [act[n, j, i : i + R].reshape(R * W, HALF) for n in range(2)], axis=1
                )
                d = jnp.dot(lhs, w1[half, 3 * i + j], preferred_element_type=F32)
                acc = d if acc is None else acc + d
        v = acc + cbias[0, half]
        h[half] = v.reshape(R, W, HALF)
        hsend[half, 0] = v[:W].astype(BF16)
        hsend[half, 1] = v[R * W - W :].astype(BF16)
        copies = halo(
            hsend.at[half, 1], hsend.at[half, 0], hrecv.at[half, 0], hrecv.at[half, 1], hh_sem.at[half]
        )
        send_stats(1 + half, *partial_sums(v))
        start_down(copies)
        start_up(copies)
        return 0

    lax.fori_loop(0, 2, h_half, 0)

    def h_norm(half):
        scale, shift = norm_terms(
            1 + half, stat_copies(stbuf.at[1 + half], 1 + half), params[2, 2 * half : 2 * half + 2], params[3, 2 * half : 2 * half + 2]
        )

        def h_line(r, _):
            put_line(r + 1, h[half, r], scale, shift, (half,))
            return 0

        lax.fori_loop(0, R, h_line, 0)
        halo_lines(hh[half], hrecv.at[half, 0], hrecv.at[half, 1], scale, shift, (half,))

    h_norm(0)
    c_w2.wait()

    yh = halo(ysend.at[1], ysend.at[0], yrecv.at[0], yrecv.at[1], yh_sem)

    def y_part(b, lo, hi, acc, s, q):
        res = jnp.concatenate(
            [vid[pl.ds(lo + 1, 2)].reshape(2 * W, C), vid[pl.ds(hi + 1, 2)].reshape(2 * W, C)],
            axis=0,
        )
        v = res.astype(F32) + (acc + jnp.concatenate([cbias[1, 0], cbias[1, 1]], axis=1))
        yp[pl.ds(lo, 2)] = v[: 2 * W].reshape(2, W, C)
        yp[pl.ds(hi, 2)] = v[2 * W :].reshape(2, W, C)
        return s, q

    def y_lines(b, lo, hi, acc, s, q):
        part = jnp.concatenate(
            [yp[pl.ds(lo, 2)].reshape(2 * W, C), yp[pl.ds(hi, 2)].reshape(2 * W, C)], axis=0
        )
        v = part + acc
        for half in range(2):
            x = v[:, HALF * half : HALF * half + HALF]
            h[half, pl.ds(lo, 2)] = x[: 2 * W].reshape(2, W, HALF)
            h[half, pl.ds(hi, 2)] = x[2 * W :].reshape(2, W, HALF)

        @pl.when(b == 0)
        def _():
            ysend[0] = v[:W].astype(BF16)
            ysend[1] = v[3 * W :].astype(BF16)
            start_down(yh)
            start_up(yh)

        a, c = partial_sums(v)
        return s + a, q + c

    conv(lambda j, line: two_lines(0, j, line), lambda tap: w2[tap, 0:HALF], C, y_part)

    h_norm(1)

    s, q = conv(lambda j, line: two_lines(1, j, line), lambda tap: w2[tap, HALF:C], C, y_lines)

    copies = send_stats(3, s, q)
    finish([c_ow] + c_q + c_tp)
    nt = (((1,), (1,)), ((), ()))
    pt[...] = jnp.zeros(pt.shape, F32)
    for t in range(3):
        for dst in (w1r, w2r):
            dst[t, 3, :, 0:T] = jnp.zeros((3 * T, T), BF16)
            dst[t, 0, :, T : 2 * T] = jnp.zeros((3 * T, T), BF16)
    row = lax.broadcasted_iota(jnp.int32, (48, 8 * R), 0)
    col = lax.broadcasted_iota(jnp.int32, (48, 8 * R), 1)
    quant = jnp.zeros((48, 8 * R), F32)
    for m in range(8):
        for c in range(4):
            hit = (row % 5 == c) & (col % 8 == m) & (row // 5 == col // 8)
            quant = quant + jnp.where(hit, qwv[c : c + 1, m : m + 1], 0.0)
    row8 = lax.broadcasted_iota(jnp.int32, (8 * R, 1), 0)
    row5 = lax.broadcasted_iota(jnp.int32, (48, 1), 0)
    head_bias = jnp.zeros((8 * R, 1), F32)
    for m in range(8):
        head_bias = head_bias + jnp.where(row8 % 8 == m, obv[0:1, m : m + 1], 0.0)
    quant_bias = jnp.zeros((48, 1), F32)
    for c in range(4):
        quant_bias = quant_bias + jnp.where(row5 % 5 == c, qbv[0:1, c : c + 1], 0.0)

    scale, shift = norm_terms(3, copies, params[4], params[5])

    def y_line(r, _):
        v = jnp.concatenate([h[0, r], h[1, r]], axis=1)
        put_line(r + 1, v, scale, shift, shifted=False)
        return 0

    lax.fori_loop(0, R, y_line, 0)
    halo_lines(yh, yrecv.at[0], yrecv.at[1], scale, shift, shifted=False)

    for r in range(R + 2):
        line = jnp.concatenate([act[0, 1, r], act[1, 1, r]], axis=1)
        pt[r, :, 0:W] = lax.dot_general(wht[...], line, nt, preferred_element_type=F32)
    for r in range(R):
        sums = []
        for j in range(3):
            x = None
            for i in range(3):
                top = 8 * (3 * i + j)
                p = pt[r + i, top : top + 8, :]
                x = p if x is None else x + p
            sums.append(x)
        mom[8 * r : 8 * r + 8] = (
            sums[1] + pltpu.roll(sums[0], 1, 1) + pltpu.roll(sums[2], LANES - 1, 1)
        )
    means = (
        jnp.dot(quant, mom[...] + head_bias, precision=lax.Precision.HIGHEST, preferred_element_type=F32)
        + quant_bias
    )
    means = LATENT_SCALE * means
    row = lax.broadcasted_iota(jnp.int32, (48, 128), 0)
    lane = lax.broadcasted_iota(jnp.int32, (48, 128), 1)
    rest = jnp.where((lane < W - 128) & (row < 5 * R), means[:, 128:256], 0.0)
    packed = jnp.where(row % 5 < 4, means[:, 0:128], 0.0)
    for c in range(4):
        moved = pltpu.roll(jnp.where(row % 5 == c, rest, 0.0), 4 - c, 0)
        packed = packed + (pltpu.roll(moved, 32 * c, 1) if c else moved)
    packed = jnp.where(row < 5 * R, packed, 0.0)
    latsend[0:48] = packed.astype(BF16)
    latsend[48:64] = pltpu.roll(packed, 48 - 25, 0)[0:16].astype(BF16)
    lx[0, 16:64] = packed.astype(BF16)

    def lat_copy(k, d):
        src = {0: pl.ds(0, 48), 1: pl.ds(48, 16), -1: pl.ds(0, 16)}[d]
        at = {0: pl.ds(16, 48), 1: pl.ds(0, 16), -1: pl.ds(64, 16)}[d]
        return pltpu.make_async_remote_copy(
            src_ref=latsend.at[src], dst_ref=lx.at[k, at],
            send_sem=lat_send.at[k, d + 1], recv_sem=lat_recv.at[k, d + 1],
            device_id={"frames": f + k, "rows": rr + d}, device_id_type=MESH,
        )

    for k, d in lat_targets():
        @pl.when(sends_to(k, d))
        def _():
            lat_copy(k, d).start()

    slot = lax.broadcasted_iota(jnp.int32, (SLOTS, 128), 0)
    lowest = jnp.where(has_above, 0, 16)
    highest = jnp.where(has_below, SLOTS, 64)
    column = lax.broadcasted_iota(jnp.int32, (W, 128), 0)
    lane = lax.broadcasted_iota(jnp.int32, (W, 128), 1)
    lane32 = lax.broadcasted_iota(jnp.int32, (32, 128), 1)
    fifth = lane32 < 0
    for line in range(-3, R + 3):
        fifth = fifth | (lane32 == packed_row(line) + 4)

    def take_latent(k, dirs=(-1, 0, 1)):
        for d in dirs:
            @pl.when(gets_from(k, d))
            def _():
                lat_copy(k, d).wait_recv()
        keep = (slot >= jnp.where(f >= k, lowest, SLOTS)) & (slot < highest)
        x = jnp.where(keep, lx[k].astype(F32), 0.0)
        x = jnp.transpose(jnp.concatenate([x, jnp.zeros((128 - SLOTS, 128), F32)], axis=0))
        rest = jnp.zeros((32, 128), F32)
        for c in range(4):
            rest = rest + pltpu.roll(jnp.where(fifth, x[32 * c : 32 * c + 32], 0.0), 128 + c - 4, 1)
        x = jnp.concatenate([x, rest], axis=0)
        left = jnp.where(column == 0, 0.0, pltpu.roll(x, 1, 0))
        right = jnp.where(column == W - 1, 0.0, pltpu.roll(x, W - 1, 0))
        centre = pltpu.roll(x, SLOTS, 1)
        ltt[k, :, 0:128] = jnp.where(lane < SLOTS, left, centre).astype(BF16)
        ltt[k, :, 128:256] = jnp.where(lane < 2 * SLOTS - 128, centre, pltpu.roll(right, 2 * SLOTS - 128, 1)).astype(BF16)

    def send_time_stats(e, s, q):
        tstbuf[e, rr, 0:1] = jnp.sum(s, axis=0, keepdims=True)
        tstbuf[e, rr, 1:2] = jnp.sum(q, axis=0, keepdims=True)
        begin(stat_copies(tstbuf.at[e], 4 + e))

    def time_terms(e, gain, shift):
        finish(stat_copies(tstbuf.at[e], 4 + e))
        total = tstbuf[e, 0]
        for r in range(1, n_rows):
            total = total + tstbuf[e, r]
        total = lane_group_sum(total, T // GROUPS) * (1.0 / (n_rows * R * W * (T // GROUPS)))
        mean = total[0:1]
        var = jnp.maximum(total[1:2] - mean * mean, 0.0)
        scale = lax.rsqrt(var + EPS) * gain
        return 0.5 * scale, 0.5 * (shift - mean * scale)

    def time_line(dst, g, n, v, scale, shift):
        for j, x in enumerate(column_shifts(half_silu(v, scale, shift))):
            dst[g, n, :, T * j : T * j + T] = x

    def pair_lines(src, g, i, pairs):
        return jnp.concatenate([src[g, 2 * p + i] for p in range(pairs)], axis=0)

    take_latent(0, (-1, 1))
    take_latent(1)

    def t0_frame(g, _):
        take_latent(g + 2)
        lhs = jnp.concatenate([ltt[g + 2], ltt[g + 1], ltt[g]], axis=1)
        s = jnp.zeros((8, T), F32)
        q = jnp.zeros((8, T), F32)
        acc = jnp.dot(lhs, wb[...], preferred_element_type=F32)
        for n in range(R + 2):
            v = acc[:, T * n : T * n + T] + tparams[0]
            t0s[g, n] = v
            if 1 <= n < R + 1:
                a, c = partial_sums(v)
                s += a
                q += c
        send_time_stats(g, s, q)
        return 0

    lax.fori_loop(0, 5, t0_frame, 0)

    finish(c_t)

    def b1_frame(g):
        scale, shift = time_terms(g, tparams[1], tparams[2])

        def lines(m, _):
            for n in (2 * m, 2 * m + 1):
                at = R * rr + n - 1
                ok = jnp.logical_and(jnp.logical_and(at >= 0, at < n_rows * R), f >= g)
                time_line(b1, g, n, t0s[g, n], jnp.where(ok, scale, 0.0), jnp.where(ok, shift, 0.0))
            return 0

        lax.fori_loop(0, R // 2 + 1, lines, 0)

    def b1_first(g, _):
        b1_frame(g)
        return 0

    lax.fori_loop(0, 2, b1_first, 0)

    pairs = R // 2

    def th(g):
        return halo(
            t1send.at[g, 1], t1send.at[g, 0], t1recv.at[g, 0], t1recv.at[g, 1], th_sem.at[g]
        )

    def t1_frame(g, _):
        b1_frame(g + 2)
        lhs = jnp.concatenate(
            [pair_lines(b1, g + 2 - t, i, pairs) for t in range(3) for i in range(4)], axis=1
        )
        acc = jnp.dot(lhs, w1r[...].reshape(12 * 3 * T, 2 * T), preferred_element_type=F32)
        s = jnp.zeros((8, T), F32)
        q = jnp.zeros((8, T), F32)
        for p in range(pairs):
            for half in range(2):
                v = acc[W * p : W * p + W, T * half : T * half + T]
                t1s[g, 2 * p + half] = v
                if 2 * p + half in (0, R - 1):
                    t1send[g, half] = v.astype(BF16)
                a, c = partial_sums(v)
                s += a
                q += c
        send_time_stats(5 + g, s, q)
        start_down(th(g))
        start_up(th(g))
        return 0

    lax.fori_loop(0, 3, t1_frame, 0)

    for p in range(R // 2):
        for half in range(2):
            facc[W * p : W * p + W, T * half : T * half + T] = t0s[0, 2 * p + half + 1] + tparams[5]

    def feature_frame(g, _):
        scale, shift = time_terms(5 + g, tparams[3], tparams[4])
        scale = jnp.where(f >= g, scale, 0.0)
        shift = jnp.where(f >= g, shift, 0.0)

        def lines(m, _):
            for n in (2 * m, 2 * m + 1):
                time_line(b2, g, n + 1, t1s[g, n], scale, shift)
            return 0

        lax.fori_loop(0, R // 2, lines, 0)
        for has, copy, side, n in ((has_above, th(g)[0], 0, 0), (has_below, th(g)[1], 1, R + 1)):
            @pl.when(has)
            def _():
                copy.wait_recv()
                time_line(b2, g, n, t1recv[g, side].astype(F32), scale, shift)

            @pl.when(jnp.logical_not(has))
            def _():
                b2[g, n] = jnp.zeros((W, 3 * T), BF16)

        lhs = jnp.concatenate([pair_lines(b2, g, i, R // 2) for i in range(4)], axis=1)
        facc[...] += jnp.dot(
            lhs, w2r[2 - g].reshape(4 * 3 * T, 2 * T), preferred_element_type=F32
        )
        return 0

    lax.fori_loop(0, 3, feature_frame, 0)

    for p in range(R // 2):
        for half in range(2):
            out[2 * p + half] = facc[W * p : W * p + W, T * half : T * half + T].astype(BF16)
    end_sends(vh)
    end_sends(hh[0])
    end_sends(hh[1])
    end_sends(yh)
    for g in range(3):
        end_sends(th(g))
    for k, d in lat_targets():
        @pl.when(sends_to(k, d))
        def _():
            lat_copy(k, d).wait_send()


def body(
    video, norm1_gain, norm1_shift, conv1_weight, conv1_bias, norm2_gain, norm2_shift,
    conv2_weight, conv2_bias, out_gain, out_shift, out_weight, out_bias, quant_weight,
    quant_bias, time_in_weight, time_in_bias, tnorm1_gain, tnorm1_shift, time1_weight,
    tnorm2_gain, tnorm2_shift, time2_weight, time2_bias, *, n_frames, n_rows,
):
    tile = lambda a: a.reshape(4, 128)
    flat = lambda a: a.reshape(1, -1)
    args = (
        video.reshape(R, W, C),
        tile(norm1_gain), tile(norm1_shift), conv1_weight.reshape(9, C, C), flat(conv1_bias),
        tile(norm2_gain), tile(norm2_shift), conv2_weight.reshape(9, C, C), flat(conv2_bias),
        tile(out_gain), tile(out_shift), out_weight.transpose(0, 1, 3, 2).reshape(72, C), flat(out_bias),
        quant_weight.T, flat(quant_bias), time_in_weight, flat(time_in_bias),
        flat(tnorm1_gain), flat(tnorm1_shift), time1_weight.reshape(3, 3, 3 * T, T),
        flat(tnorm2_gain), flat(tnorm2_shift), time2_weight.reshape(3, 3, 3 * T, T),
        flat(time2_bias),
    )
    vmem = lambda *shape, dtype=BF16: pltpu.VMEM(shape, dtype)
    dma = pltpu.SemaphoreType.DMA
    result = pl.pallas_call(
        functools.partial(kernel, n_frames, n_rows),
        out_shape=pltpu.VMEM((R, W, T), BF16),
        in_specs=[pl.BlockSpec(memory_space=pl.ANY)] * len(args),
        out_specs=pl.BlockSpec(memory_space=pltpu.VMEM),
        scratch_shapes=[
            vmem(R + 2, W, C),
            vmem(2, 9, C, HALF),
            vmem(9, C, C),
            vmem(2, 3, R + 2, W, HALF),
            vmem(2, R, W, HALF, dtype=F32),
            vmem(R, W, C, dtype=F32),
            vmem(2, 2, W, HALF),
            vmem(2, 2, W, HALF),
            vmem(2, W, C),
            vmem(2, W, C),
            vmem(6, 4, 128, dtype=F32),
            vmem(2, 2, 1, HALF, dtype=F32),
            vmem(6, 1, T, dtype=F32),
            vmem(1, 8, dtype=F32),
            vmem(4, 8, dtype=F32),
            vmem(1, 4, dtype=F32),
            vmem(3, 3, 3, 4, T),
            vmem(72, C),
            vmem(R + 2, 72, LANES, dtype=F32),
            vmem(8 * R, LANES, dtype=F32),
            vmem(256, (R + 2) * T, dtype=F32),
            vmem(768, (R + 2) * T),
            vmem(3, 4, 3 * T, 2 * T),
            vmem(3, 4, 3 * T, 2 * T),
            vmem(4, n_rows, 8, 128, dtype=F32),
            vmem(8, n_rows, 8, 128, dtype=F32),
            vmem(64, 128),
            vmem(BACK + 1, SLOTS, 128),
            vmem(BACK + 1, W, 256),
            vmem(5, R + 2, W, T, dtype=F32),
            vmem(5, R + 2, W, 3 * T),
            vmem(3, R, W, T, dtype=F32),
            vmem(3, 2, W, T),
            vmem(3, 2, W, T),
            vmem(3, R + 2, W, 3 * T),
            vmem(R // 2 * W, 2 * T, dtype=F32),
            dma((29,)),
            dma((4,)),
            dma((2, 4)),
            dma((4,)),
            dma((3, 4)),
            dma((12, 2, n_rows - 1)),
            dma((BACK + 1, 3)),
            dma((BACK + 1, 3)),
        ],
        compiler_params=pltpu.CompilerParams(
            collective_id=0, has_side_effects=True, vmem_limit_bytes=60 * 1024 * 1024
        ),
        name="encoder_window",
    )(*args)
    return result[None]


def solution(mesh):
    step = functools.partial(body, n_frames=mesh.shape["frames"], n_rows=mesh.shape["rows"])
    return jax.shard_map(
        step,
        mesh=mesh,
        in_specs=(P("frames", "rows", None, None),) + (P(),) * 23,
        out_specs=P("frames", "rows", None, None),
        check_vma=False,
    )
```

```python
import functools

import jax
import jax.numpy as jnp
from jax import lax
from jax.experimental import pallas as pl
from jax.experimental.pallas import tpu as pltpu
from jax.sharding import PartitionSpec as P

GROUPS = 32
EPS = 1e-06
LATENT_SCALE = 0.13025

R = 8
W = 160
C = 512
T = 128
HALF = C // 2
LANES = 256
SLOTS = 80
BACK = 6

MESH = pl.DeviceIdType.MESH
F32 = jnp.float32
BF16 = jnp.bfloat16


def lane_group_sum(x, size):
    lane = lax.broadcasted_iota(jnp.int32, x.shape, 1)
    step = 1
    while step < size:
        up = pltpu.roll(x, step, 1)
        down = pltpu.roll(x, 128 - step, 1)
        x = x + jnp.where((lane // step) % 2 == 1, up, down)
        step *= 2
    return x


def column_shifts(a):
    row = lax.broadcasted_iota(jnp.int32, (8, a.shape[1]), 0)
    left = pltpu.roll(a, 1, 0)
    left = jnp.concatenate([jnp.where(row == 0, 0.0, left[:8]), left[8:]], axis=0)
    right = pltpu.roll(a, W - 1, 0)
    right = jnp.concatenate([right[: W - 8], jnp.where(row == 7, 0.0, right[W - 8 :])], axis=0)
    return left.astype(BF16), a.astype(BF16), right.astype(BF16)


def half_silu(v, scale, shift):
    w = v * scale + shift
    return w * jnp.tanh(w) + w


def packed_row(line):
    if line < 0:
        return 5 * (line + 3)
    if line < R:
        return 16 + 5 * line
    return 64 + 5 * (line - R)


def partial_sums(v):
    g = v.reshape(-1, 8, v.shape[-1])
    return jnp.sum(g, axis=0), jnp.sum(g * g, axis=0)


def kernel(
    n_frames,
    n_rows,
    video, g1, s1, cw1, cb1, g2, s2, cw2, cb2, g3, s3, ow, ob, qw, qb,
    tiw, tib, tg1, ts1, tw1, tg2, ts2, tw2, tb2,
    out,
    vid, w1, w2, act, h, yp, hsend, hrecv, ysend, yrecv,
    params, cbias, tparams, obv, qwv, qbv, tiwv,
    wht, pt, mom, wbf, wb, w1r, w2r,
    stbuf, tstbuf, latsend, lx, ltt, t0s, b1, t1s, t1send, t1recv, b2, facc,
    in_sem, vh_sem, hh_sem, yh_sem, th_sem, st_sem, lat_send, lat_recv,
):
    f = lax.axis_index("frames")
    rr = lax.axis_index("rows")

    def local(src, dst, k):
        return pltpu.make_async_copy(src, dst, in_sem.at[k])

    c_vid = local(video, vid.at[pl.ds(1, R)], 0)
    c_w1 = [local(cw1.at[:, :, pl.ds(HALF * i, HALF)], w1.at[i], (1, 26)[i]) for i in range(2)]
    c_w2 = [local(cw2.at[:, :, pl.ds(HALF * i, HALF)], w2.at[i], (2, 29)[i]) for i in range(2)]
    c_par = [local(a, params.at[i], 3 + i) for i, a in enumerate((g1, s1, g2, s2, g3, s3))]
    c_cb = [
        local(a.at[:, pl.ds(HALF * n, HALF)], cbias.at[i, n], (9, 27)[n] + i)
        for i, a in enumerate((cb1, cb2))
        for n in range(2)
    ]
    c_tp = [local(a, tparams.at[i], 11 + i) for i, a in enumerate((tib, tg1, ts1, tg2, ts2, tb2))]
    c_ow = local(ow, wht, 17)
    c_q = [local(ob, obv, 18), local(qw, qwv, 19), local(qb, qbv, 20)]
    c_tiw = local(tiw, tiwv, 21)
    c_t = []
    for i, (src, dst) in enumerate(((tw1, w1r), (tw2, w2r))):
        for p in range(2):
            c_t.append(local(src, dst.at[:, pl.ds(p, 3), :, pl.ds(T * p, T)], 22 + 2 * i + p))

    def begin(copies):
        for c in copies:
            c.start()

    def finish(copies):
        for c in copies:
            c.wait()

    def lat_targets():
        for k in range(BACK + 1):
            for d in (-1, 0, 1):
                if k or d:
                    yield k, d

    def sends_to(k, d):
        ok = f + k < n_frames
        if d == -1:
            ok = jnp.logical_and(ok, rr > 0)
        if d == 1:
            ok = jnp.logical_and(ok, rr < n_rows - 1)
        return ok

    def gets_from(k, d):
        ok = f >= k
        if d == -1:
            ok = jnp.logical_and(ok, rr < n_rows - 1)
        if d == 1:
            ok = jnp.logical_and(ok, rr > 0)
        return ok

    c_vid.start()
    stbuf[...] = jnp.zeros(stbuf.shape, F32)
    tstbuf[...] = jnp.zeros(tstbuf.shape, F32)
    barrier = pltpu.get_barrier_semaphore()
    for d in range(1, n_rows):
        pl.semaphore_signal(
            barrier, inc=1, device_id={"frames": f, "rows": lax.rem(rr + d, n_rows)},
            device_id_type=MESH,
        )
    for k, d in lat_targets():
        if k:
            @pl.when(gets_from(k, d))
            def _():
                pl.semaphore_signal(
                    barrier, inc=1, device_id={"frames": f - k, "rows": rr - d}, device_id_type=MESH
                )

    begin(c_par + c_cb + c_tp + [c_ow] + c_q + [c_tiw])

    def halo(src_last, src_first, dst_above, dst_below, sem):
        down = pltpu.make_async_remote_copy(
            src_ref=src_last, dst_ref=dst_above, send_sem=sem.at[0], recv_sem=sem.at[1],
            device_id={"frames": f, "rows": rr + 1}, device_id_type=MESH,
        )
        up = pltpu.make_async_remote_copy(
            src_ref=src_first, dst_ref=dst_below, send_sem=sem.at[2], recv_sem=sem.at[3],
            device_id={"frames": f, "rows": rr - 1}, device_id_type=MESH,
        )
        return down, up

    has_above = rr > 0
    has_below = rr < n_rows - 1

    def stat_copies(buf, e):
        return [
            pltpu.make_async_remote_copy(
                src_ref=buf.at[rr], dst_ref=buf.at[rr],
                send_sem=st_sem.at[e, 0, d - 1], recv_sem=st_sem.at[e, 1, d - 1],
                device_id={"frames": f, "rows": lax.rem(rr + d, n_rows)}, device_id_type=MESH,
            )
            for d in range(1, n_rows)
        ]

    def send_stats(e, s, q):
        s = jnp.sum(s, axis=0, keepdims=True)
        q = jnp.sum(q, axis=0, keepdims=True)
        tiles = s.shape[1] // 128
        for t in range(tiles):
            stbuf[e, rr, t : t + 1, :] = s[:, 128 * t : 128 * t + 128]
            stbuf[e, rr, tiles + t : tiles + t + 1, :] = q[:, 128 * t : 128 * t + 128]
        copies = stat_copies(stbuf.at[e], e)
        begin(copies)
        return copies

    def norm_terms(e, copies, gain, shift):
        finish(copies)
        tiles = gain.shape[0]
        total = stbuf[e, 0]
        for r in range(1, n_rows):
            total = total + stbuf[e, r]
        total = lane_group_sum(total, C // GROUPS) * (1.0 / (n_rows * R * W * (C // GROUPS)))
        mean = total[0:tiles]
        var = jnp.maximum(total[tiles : 2 * tiles] - mean * mean, 0.0)
        scale = lax.rsqrt(var + EPS) * gain
        shift = shift - mean * scale
        wide = lambda x: jnp.concatenate([x[t : t + 1] for t in range(tiles)], axis=1) * 0.5
        return wide(scale), wide(shift)

    def put_line(line, v, scale, shift, halves=(0, 1), shifted=True):
        a = half_silu(v, scale, shift)
        taps = column_shifts(a) if shifted else (None, a.astype(BF16), None)
        for j, x in enumerate(taps):
            if x is not None:
                for n, half in enumerate(halves):
                    act[half, j, line] = x[:, HALF * n : HALF * n + HALF]

    def halo_lines(copies, above, below, scale, shift, halves=(0, 1), shifted=True):
        taps = range(3) if shifted else (1,)
        for has, copy, ref, line in (
            (has_above, copies[0], above, 0),
            (has_below, copies[1], below, R + 1),
        ):
            @pl.when(has)
            def _():
                copy.wait_recv()
                put_line(line, ref[...].astype(F32), scale, shift, halves, shifted)

            @pl.when(jnp.logical_not(has))
            def _():
                for half in halves:
                    for j in taps:
                        act[half, j, line] = jnp.zeros((W, HALF), BF16)

    def start_down(copies):
        @pl.when(has_below)
        def _():
            copies[0].start()

    def start_up(copies):
        @pl.when(has_above)
        def _():
            copies[1].start()

    def end_sends(copies):
        @pl.when(has_below)
        def _():
            copies[0].wait_send()

        @pl.when(has_above)
        def _():
            copies[1].wait_send()

    def conv(lhs_of, weight_of, width, finish_lines):
        def block(b, carry):
            s, q = carry
            lo = 2 * b
            hi = R - 2 - 2 * b
            acc = None
            for i in range(3):
                for j in range(3):
                    lhs = jnp.concatenate([lhs_of(j, lo + i), lhs_of(j, hi + i)], axis=0)
                    d = jnp.dot(lhs, weight_of(3 * i + j), preferred_element_type=F32)
                    acc = d if acc is None else acc + d
            return finish_lines(b, lo, hi, acc, s, q)

        zero = jnp.zeros((8, width), F32)
        return lax.fori_loop(0, 2, block, (zero, zero))

    def two_lines(half, j, line):
        return act[half, j, pl.ds(line, 2)].reshape(2 * W, HALF)

    c_vid.wait()
    begin(c_w1)

    def video_sums(r, carry):
        s, q = carry
        a, b = partial_sums(vid[r + 1].astype(F32))
        return s + a, q + b

    zero = jnp.zeros((8, C), F32)
    s, q = lax.fori_loop(0, R, video_sums, (zero, zero))

    later = sum(1 - lax.div(f + k, n_frames) for k in range(1, BACK + 1))
    lines = 2 + lax.div(rr + n_rows - 1, n_rows) - lax.div(rr + 1, n_rows)
    pl.semaphore_wait(barrier, n_rows - 1 + later * lines)

    copies = send_stats(0, s, q)
    vh = halo(vid.at[R], vid.at[1], vid.at[0], vid.at[R + 1], vh_sem)
    start_down(vh)
    start_up(vh)
    begin(c_w2)
    begin(c_t)

    finish([c_tiw])
    wbf[...] = jnp.zeros(wbf.shape, F32)
    for t in range(3):
        for j in range(3):
            for i in range(3):
                piece = tiwv[t, i, j].astype(F32)
                for n in range(R + 2):
                    top = SLOTS * j + packed_row(n + i - 2)
                    wbf[top : top + 4, T * n : T * n + T] = piece
        wb[256 * t : 256 * t + 256] = wbf[...].astype(BF16)

    finish(c_par + c_cb)
    scale, shift = norm_terms(0, copies, params[0], params[1])

    def video_line(r, _):
        put_line(r + 1, vid[r + 1].astype(F32), scale, shift)
        return 0

    lax.fori_loop(0, R, video_line, 0)
    halo_lines(vh, vid.at[0], vid.at[R + 1], scale, shift)
    finish(c_w1)

    hh = [halo(hsend.at[i, 1], hsend.at[i, 0], hrecv.at[i, 0], hrecv.at[i, 1], hh_sem.at[i]) for i in range(2)]

    def h_half(half, _):
        acc = None
        for i in range(3):
            for j in range(3):
                lhs = jnp.concatenate(
                    [act[n, j, i : i + R].reshape(R * W, HALF) for n in range(2)], axis=1
                )
                d = jnp.dot(lhs, w1[half, 3 * i + j], preferred_element_type=F32)
                acc = d if acc is None else acc + d
        v = acc + cbias[0, half]
        h[half] = v.reshape(R, W, HALF)
        hsend[half, 0] = v[:W].astype(BF16)
        hsend[half, 1] = v[R * W - W :].astype(BF16)
        copies = halo(
            hsend.at[half, 1], hsend.at[half, 0], hrecv.at[half, 0], hrecv.at[half, 1], hh_sem.at[half]
        )
        send_stats(1 + half, *partial_sums(v))
        start_down(copies)
        start_up(copies)
        return 0

    lax.fori_loop(0, 2, h_half, 0)

    def h_norm(half):
        scale, shift = norm_terms(
            1 + half, stat_copies(stbuf.at[1 + half], 1 + half), params[2, 2 * half : 2 * half + 2], params[3, 2 * half : 2 * half + 2]
        )

        def h_line(r, _):
            put_line(r + 1, h[half, r], scale, shift, (half,))
            return 0

        lax.fori_loop(0, R, h_line, 0)
        halo_lines(hh[half], hrecv.at[half, 0], hrecv.at[half, 1], scale, shift, (half,))

    h_norm(0)
    finish(c_w2)

    yh = [halo(ysend.at[i, 1], ysend.at[i, 0], yrecv.at[i, 0], yrecv.at[i, 1], yh_sem.at[i]) for i in range(2)]

    def y_part(b, lo, hi, acc, s, q):
        res = jnp.concatenate(
            [vid[pl.ds(lo + 1, 2)].reshape(2 * W, C), vid[pl.ds(hi + 1, 2)].reshape(2 * W, C)],
            axis=0,
        )
        v = res.astype(F32) + (acc + jnp.concatenate([cbias[1, 0], cbias[1, 1]], axis=1))
        for half in range(2):
            x = v[:, HALF * half : HALF * half + HALF]
            yp[half, pl.ds(lo, 2)] = x[: 2 * W].reshape(2, W, HALF)
            yp[half, pl.ds(hi, 2)] = x[2 * W :].reshape(2, W, HALF)
        return s, q

    conv(lambda j, line: two_lines(0, j, line), lambda tap: jnp.concatenate([w2[0, tap, 0:HALF], w2[1, tap, 0:HALF]], axis=1), C, y_part)

    h_norm(1)

    def y_half(half, _):
        acc = None
        for i in range(3):
            for j in range(3):
                lhs = act[1, j, i : i + R].reshape(R * W, HALF)
                d = jnp.dot(lhs, w2[half, 3 * i + j, HALF:C], preferred_element_type=F32)
                acc = d if acc is None else acc + d
        v = yp[half].reshape(R * W, HALF) + acc
        h[half] = v.reshape(R, W, HALF)
        ysend[half, 0] = v[:W].astype(BF16)
        ysend[half, 1] = v[R * W - W :].astype(BF16)
        copies = halo(
            ysend.at[half, 1], ysend.at[half, 0], yrecv.at[half, 0], yrecv.at[half, 1], yh_sem.at[half]
        )
        send_stats(3 + half, *partial_sums(v))
        start_down(copies)
        start_up(copies)
        return 0

    lax.fori_loop(0, 2, y_half, 0)

    finish([c_ow] + c_q + c_tp)
    nt = (((1,), (1,)), ((), ()))
    pt[...] = jnp.zeros(pt.shape, F32)
    for t in range(3):
        for dst in (w1r, w2r):
            dst[t, 3, :, 0:T] = jnp.zeros((3 * T, T), BF16)
            dst[t, 0, :, T : 2 * T] = jnp.zeros((3 * T, T), BF16)
    row = lax.broadcasted_iota(jnp.int32, (48, 8 * R), 0)
    col = lax.broadcasted_iota(jnp.int32, (48, 8 * R), 1)
    quant = jnp.zeros((48, 8 * R), F32)
    for m in range(8):
        for c in range(4):
            hit = (row % 5 == c) & (col % 8 == m) & (row // 5 == col // 8)
            quant = quant + jnp.where(hit, qwv[c : c + 1, m : m + 1], 0.0)
    row8 = lax.broadcasted_iota(jnp.int32, (8 * R, 1), 0)
    row5 = lax.broadcasted_iota(jnp.int32, (48, 1), 0)
    head_bias = jnp.zeros((8 * R, 1), F32)
    for m in range(8):
        head_bias = head_bias + jnp.where(row8 % 8 == m, obv[0:1, m : m + 1], 0.0)
    quant_bias = jnp.zeros((48, 1), F32)
    for c in range(4):
        quant_bias = quant_bias + jnp.where(row5 % 5 == c, qbv[0:1, c : c + 1], 0.0)

    def y_norm(half):
        scale, shift = norm_terms(
            3 + half, stat_copies(stbuf.at[3 + half], 3 + half),
            params[4, 2 * half : 2 * half + 2], params[5, 2 * half : 2 * half + 2],
        )

        def y_line(r, _):
            put_line(r + 1, h[half, r], scale, shift, (half,), shifted=False)
            return 0

        lax.fori_loop(0, R, y_line, 0)
        halo_lines(yh[half], yrecv.at[half, 0], yrecv.at[half, 1], scale, shift, (half,), shifted=False)

    y_norm(0)
    for r in range(R + 2):
        pt[r, :, 0:W] = lax.dot_general(wht[:, 0:HALF], act[0, 1, r], nt, preferred_element_type=F32)
    y_norm(1)
    for r in range(R + 2):
        pt[r, :, 0:W] += lax.dot_general(wht[:, HALF:C], act[1, 1, r], nt, preferred_element_type=F32)
    for r in range(R):
        sums = []
        for j in range(3):
            x = None
            for i in range(3):
                top = 8 * (3 * i + j)
                p = pt[r + i, top : top + 8, :]
                x = p if x is None else x + p
            sums.append(x)
        mom[8 * r : 8 * r + 8] = (
            sums[1] + pltpu.roll(sums[0], 1, 1) + pltpu.roll(sums[2], LANES - 1, 1)
        )
    means = (
        jnp.dot(quant, mom[...] + head_bias, precision=lax.Precision.HIGHEST, preferred_element_type=F32)
        + quant_bias
    )
    means = LATENT_SCALE * means
    row = lax.broadcasted_iota(jnp.int32, (48, 128), 0)
    lane = lax.broadcasted_iota(jnp.int32, (48, 128), 1)
    rest = jnp.where((lane < W - 128) & (row < 5 * R), means[:, 128:256], 0.0)
    packed = jnp.where(row % 5 < 4, means[:, 0:128], 0.0)
    for c in range(4):
        moved = pltpu.roll(jnp.where(row % 5 == c, rest, 0.0), 4 - c, 0)
        packed = packed + (pltpu.roll(moved, 32 * c, 1) if c else moved)
    packed = jnp.where(row < 5 * R, packed, 0.0)
    latsend[0:48] = packed.astype(BF16)
    latsend[48:64] = pltpu.roll(packed, 48 - 25, 0)[0:16].astype(BF16)
    lx[0, 16:64] = packed.astype(BF16)

    def lat_copy(k, d):
        src = {0: pl.ds(0, 48), 1: pl.ds(48, 16), -1: pl.ds(0, 16)}[d]
        at = {0: pl.ds(16, 48), 1: pl.ds(0, 16), -1: pl.ds(64, 16)}[d]
        return pltpu.make_async_remote_copy(
            src_ref=latsend.at[src], dst_ref=lx.at[k, at],
            send_sem=lat_send.at[k, d + 1], recv_sem=lat_recv.at[k, d + 1],
            device_id={"frames": f + k, "rows": rr + d}, device_id_type=MESH,
        )

    for k, d in lat_targets():
        @pl.when(sends_to(k, d))
        def _():
            lat_copy(k, d).start()

    slot = lax.broadcasted_iota(jnp.int32, (SLOTS, 128), 0)
    lowest = jnp.where(has_above, 0, 16)
    highest = jnp.where(has_below, SLOTS, 64)
    column = lax.broadcasted_iota(jnp.int32, (W, 128), 0)
    lane = lax.broadcasted_iota(jnp.int32, (W, 128), 1)
    lane32 = lax.broadcasted_iota(jnp.int32, (32, 128), 1)
    fifth = lane32 < 0
    for line in range(-3, R + 3):
        fifth = fifth | (lane32 == packed_row(line) + 4)

    def take_latent(k, dirs=(-1, 0, 1)):
        for d in dirs:
            @pl.when(gets_from(k, d))
            def _():
                lat_copy(k, d).wait_recv()
        keep = (slot >= jnp.where(f >= k, lowest, SLOTS)) & (slot < highest)
        x = jnp.where(keep, lx[k].astype(F32), 0.0)
        x = jnp.transpose(jnp.concatenate([x, jnp.zeros((128 - SLOTS, 128), F32)], axis=0))
        rest = jnp.zeros((32, 128), F32)
        for c in range(4):
            rest = rest + pltpu.roll(jnp.where(fifth, x[32 * c : 32 * c + 32], 0.0), 128 + c - 4, 1)
        x = jnp.concatenate([x, rest], axis=0)
        left = jnp.where(column == 0, 0.0, pltpu.roll(x, 1, 0))
        right = jnp.where(column == W - 1, 0.0, pltpu.roll(x, W - 1, 0))
        centre = pltpu.roll(x, SLOTS, 1)
        ltt[k, :, 0:128] = jnp.where(lane < SLOTS, left, centre).astype(BF16)
        ltt[k, :, 128:256] = jnp.where(lane < 2 * SLOTS - 128, centre, pltpu.roll(right, 2 * SLOTS - 128, 1)).astype(BF16)

    def send_time_stats(e, s, q):
        tstbuf[e, rr, 0:1] = jnp.sum(s, axis=0, keepdims=True)
        tstbuf[e, rr, 1:2] = jnp.sum(q, axis=0, keepdims=True)
        begin(stat_copies(tstbuf.at[e], 5 + e))

    def time_terms(e, gain, shift):
        finish(stat_copies(tstbuf.at[e], 5 + e))
        total = tstbuf[e, 0]
        for r in range(1, n_rows):
            total = total + tstbuf[e, r]
        total = lane_group_sum(total, T // GROUPS) * (1.0 / (n_rows * R * W * (T // GROUPS)))
        mean = total[0:1]
        var = jnp.maximum(total[1:2] - mean * mean, 0.0)
        scale = lax.rsqrt(var + EPS) * gain
        return 0.5 * scale, 0.5 * (shift - mean * scale)

    def time_line(dst, g, n, v, scale, shift):
        for j, x in enumerate(column_shifts(half_silu(v, scale, shift))):
            dst[g, n, :, T * j : T * j + T] = x

    def pair_lines(src, g, i, pairs):
        return jnp.concatenate([src[g, 2 * p + i] for p in range(pairs)], axis=0)

    take_latent(0, (-1, 1))
    take_latent(1)

    def t0_frame(g, _):
        take_latent(g + 2)
        lhs = jnp.concatenate([ltt[g + 2], ltt[g + 1], ltt[g]], axis=1)
        s = jnp.zeros((8, T), F32)
        q = jnp.zeros((8, T), F32)
        acc = jnp.dot(lhs, wb[...], preferred_element_type=F32)
        for n in range(R + 2):
            v = acc[:, T * n : T * n + T] + tparams[0]
            t0s[g, n] = v
            if 1 <= n < R + 1:
                a, c = partial_sums(v)
                s += a
                q += c
        send_time_stats(g, s, q)
        return 0

    lax.fori_loop(0, 5, t0_frame, 0)

    finish(c_t)

    def b1_frame(g):
        scale, shift = time_terms(g, tparams[1], tparams[2])

        def lines(m, _):
            for n in (2 * m, 2 * m + 1):
                at = R * rr + n - 1
                ok = jnp.logical_and(jnp.logical_and(at >= 0, at < n_rows * R), f >= g)
                time_line(b1, g, n, t0s[g, n], jnp.where(ok, scale, 0.0), jnp.where(ok, shift, 0.0))
            return 0

        lax.fori_loop(0, R // 2 + 1, lines, 0)

    def b1_first(g, _):
        b1_frame(g)
        return 0

    lax.fori_loop(0, 2, b1_first, 0)

    pairs = R // 2

    def th(g):
        return halo(
            t1send.at[g, 1], t1send.at[g, 0], t1recv.at[g, 0], t1recv.at[g, 1], th_sem.at[g]
        )

    def t1_frame(g, _):
        b1_frame(g + 2)
        lhs = jnp.concatenate(
            [pair_lines(b1, g + 2 - t, i, pairs) for t in range(3) for i in range(4)], axis=1
        )
        acc = jnp.dot(lhs, w1r[...].reshape(12 * 3 * T, 2 * T), preferred_element_type=F32)
        s = jnp.zeros((8, T), F32)
        q = jnp.zeros((8, T), F32)
        for p in range(pairs):
            for half in range(2):
                v = acc[W * p : W * p + W, T * half : T * half + T]
                t1s[g, 2 * p + half] = v
                if 2 * p + half in (0, R - 1):
                    t1send[g, half] = v.astype(BF16)
                a, c = partial_sums(v)
                s += a
                q += c
        send_time_stats(5 + g, s, q)
        start_down(th(g))
        start_up(th(g))
        return 0

    lax.fori_loop(0, 3, t1_frame, 0)

    for p in range(R // 2):
        for half in range(2):
            facc[W * p : W * p + W, T * half : T * half + T] = t0s[0, 2 * p + half + 1] + tparams[5]

    def feature_frame(g, _):
        scale, shift = time_terms(5 + g, tparams[3], tparams[4])
        scale = jnp.where(f >= g, scale, 0.0)
        shift = jnp.where(f >= g, shift, 0.0)

        def lines(m, _):
            for n in (2 * m, 2 * m + 1):
                time_line(b2, g, n + 1, t1s[g, n], scale, shift)
            return 0

        lax.fori_loop(0, R // 2, lines, 0)
        for has, copy, side, n in ((has_above, th(g)[0], 0, 0), (has_below, th(g)[1], 1, R + 1)):
            @pl.when(has)
            def _():
                copy.wait_recv()
                time_line(b2, g, n, t1recv[g, side].astype(F32), scale, shift)

            @pl.when(jnp.logical_not(has))
            def _():
                b2[g, n] = jnp.zeros((W, 3 * T), BF16)

        lhs = jnp.concatenate([pair_lines(b2, g, i, R // 2) for i in range(4)], axis=1)
        facc[...] += jnp.dot(
            lhs, w2r[2 - g].reshape(4 * 3 * T, 2 * T), preferred_element_type=F32
        )
        return 0

    lax.fori_loop(0, 3, feature_frame, 0)

    for p in range(R // 2):
        for half in range(2):
            out[2 * p + half] = facc[W * p : W * p + W, T * half : T * half + T].astype(BF16)
    end_sends(vh)
    end_sends(hh[0])
    end_sends(hh[1])
    end_sends(yh[0])
    end_sends(yh[1])
    for g in range(3):
        end_sends(th(g))
    for k, d in lat_targets():
        @pl.when(sends_to(k, d))
        def _():
            lat_copy(k, d).wait_send()


def body(
    video, norm1_gain, norm1_shift, conv1_weight, conv1_bias, norm2_gain, norm2_shift,
    conv2_weight, conv2_bias, out_gain, out_shift, out_weight, out_bias, quant_weight,
    quant_bias, time_in_weight, time_in_bias, tnorm1_gain, tnorm1_shift, time1_weight,
    tnorm2_gain, tnorm2_shift, time2_weight, time2_bias, *, n_frames, n_rows,
):
    tile = lambda a: a.reshape(4, 128)
    flat = lambda a: a.reshape(1, -1)
    args = (
        video.reshape(R, W, C),
        tile(norm1_gain), tile(norm1_shift), conv1_weight.reshape(9, C, C), flat(conv1_bias),
        tile(norm2_gain), tile(norm2_shift), conv2_weight.reshape(9, C, C), flat(conv2_bias),
        tile(out_gain), tile(out_shift), out_weight.transpose(0, 1, 3, 2).reshape(72, C), flat(out_bias),
        quant_weight.T, flat(quant_bias), time_in_weight, flat(time_in_bias),
        flat(tnorm1_gain), flat(tnorm1_shift), time1_weight.reshape(3, 3, 3 * T, T),
        flat(tnorm2_gain), flat(tnorm2_shift), time2_weight.reshape(3, 3, 3 * T, T),
        flat(time2_bias),
    )
    vmem = lambda *shape, dtype=BF16: pltpu.VMEM(shape, dtype)
    dma = pltpu.SemaphoreType.DMA
    result = pl.pallas_call(
        functools.partial(kernel, n_frames, n_rows),
        out_shape=pltpu.VMEM((R, W, T), BF16),
        in_specs=[pl.BlockSpec(memory_space=pl.ANY)] * len(args),
        out_specs=pl.BlockSpec(memory_space=pltpu.VMEM),
        scratch_shapes=[
            vmem(R + 2, W, C),
            vmem(2, 9, C, HALF),
            vmem(2, 9, C, HALF),
            vmem(2, 3, R + 2, W, HALF),
            vmem(2, R, W, HALF, dtype=F32),
            vmem(2, R, W, HALF, dtype=F32),
            vmem(2, 2, W, HALF),
            vmem(2, 2, W, HALF),
            vmem(2, 2, W, HALF),
            vmem(2, 2, W, HALF),
            vmem(6, 4, 128, dtype=F32),
            vmem(2, 2, 1, HALF, dtype=F32),
            vmem(6, 1, T, dtype=F32),
            vmem(1, 8, dtype=F32),
            vmem(4, 8, dtype=F32),
            vmem(1, 4, dtype=F32),
            vmem(3, 3, 3, 4, T),
            vmem(72, C),
            vmem(R + 2, 72, LANES, dtype=F32),
            vmem(8 * R, LANES, dtype=F32),
            vmem(256, (R + 2) * T, dtype=F32),
            vmem(768, (R + 2) * T),
            vmem(3, 4, 3 * T, 2 * T),
            vmem(3, 4, 3 * T, 2 * T),
            vmem(5, n_rows, 8, 128, dtype=F32),
            vmem(8, n_rows, 8, 128, dtype=F32),
            vmem(64, 128),
            vmem(BACK + 1, SLOTS, 128),
            vmem(BACK + 1, W, 256),
            vmem(5, R + 2, W, T, dtype=F32),
            vmem(5, R + 2, W, 3 * T),
            vmem(3, R, W, T, dtype=F32),
            vmem(3, 2, W, T),
            vmem(3, 2, W, T),
            vmem(3, R + 2, W, 3 * T),
            vmem(R // 2 * W, 2 * T, dtype=F32),
            dma((30,)),
            dma((4,)),
            dma((2, 4)),
            dma((2, 4)),
            dma((3, 4)),
            dma((13, 2, n_rows - 1)),
            dma((BACK + 1, 3)),
            dma((BACK + 1, 3)),
        ],
        compiler_params=pltpu.CompilerParams(
            collective_id=0, has_side_effects=True, vmem_limit_bytes=60 * 1024 * 1024
        ),
        name="encoder_window",
    )(*args)
    return result[None]


def solution(mesh):
    step = functools.partial(body, n_frames=mesh.shape["frames"], n_rows=mesh.shape["rows"])
    return jax.shard_map(
        step,
        mesh=mesh,
        in_specs=(P("frames", "rows", None, None),) + (P(),) * 23,
        out_specs=P("frames", "rows", None, None),
        check_vma=False,
    )
```

```python
import functools

import jax
import jax.numpy as jnp
from jax import lax
from jax.experimental import pallas as pl
from jax.experimental.pallas import tpu as pltpu
from jax.sharding import PartitionSpec as P

GROUPS = 32
EPS = 1e-06
LATENT_SCALE = 0.13025

R = 8
W = 160
C = 512
T = 128
HALF = C // 2
LANES = 256
SLOTS = 80
BACK = 6

MESH = pl.DeviceIdType.MESH
F32 = jnp.float32
BF16 = jnp.bfloat16


def lane_group_sum(x, size):
    lane = lax.broadcasted_iota(jnp.int32, x.shape, 1)
    step = 1
    while step < size:
        up = pltpu.roll(x, step, 1)
        down = pltpu.roll(x, 128 - step, 1)
        x = x + jnp.where((lane // step) % 2 == 1, up, down)
        step *= 2
    return x


def column_shifts(a):
    row = lax.broadcasted_iota(jnp.int32, (8, a.shape[1]), 0)
    left = pltpu.roll(a, 1, 0)
    left = jnp.concatenate([jnp.where(row == 0, 0.0, left[:8]), left[8:]], axis=0)
    right = pltpu.roll(a, W - 1, 0)
    right = jnp.concatenate([right[: W - 8], jnp.where(row == 7, 0.0, right[W - 8 :])], axis=0)
    return left.astype(BF16), a.astype(BF16), right.astype(BF16)


def half_silu(v, scale, shift):
    w = v * scale + shift
    return w * jnp.tanh(w) + w


def packed_row(line):
    if line < 0:
        return 5 * (line + 3)
    if line < R:
        return 16 + 5 * line
    return 64 + 5 * (line - R)


def partial_sums(v):
    g = v.reshape(-1, 8, v.shape[-1])
    return jnp.sum(g, axis=0), jnp.sum(g * g, axis=0)


def kernel(
    n_frames,
    n_rows,
    video, g1, s1, cw1, cb1, g2, s2, cw2, cb2, g3, s3, ow, ob, qw, qb,
    tiw, tib, tg1, ts1, tw1, tg2, ts2, tw2, tb2,
    out,
    vid, w1, w2, act, h, yp, hsend, hrecv, ysend, yrecv,
    params, cbias, tparams, obv, qwv, qbv, tiwv,
    wht, pt, mom, wbf, wb, w1r, w2r,
    stbuf, tstbuf, latsend, lx, ltt, t0s, b1, t1s, t1send, t1recv, b2, facc,
    in_sem, vh_sem, hh_sem, yh_sem, th_sem, st_sem, lat_send, lat_recv,
):
    f = lax.axis_index("frames")
    rr = lax.axis_index("rows")

    def local(src, dst, k):
        return pltpu.make_async_copy(src, dst, in_sem.at[k])

    c_vid = local(video, vid.at[pl.ds(1, R)], 0)
    c_w1 = [local(cw1.at[:, :, pl.ds(HALF * i, HALF)], w1.at[i], (1, 26)[i]) for i in range(2)]
    c_w2 = [local(cw2.at[:, :, pl.ds(HALF * i, HALF)], w2.at[i], (2, 29)[i]) for i in range(2)]
    c_par = [local(a, params.at[i], 3 + i) for i, a in enumerate((g1, s1, g2, s2, g3, s3))]
    c_cb = [
        local(a.at[:, pl.ds(HALF * n, HALF)], cbias.at[i, n], (9, 27)[n] + i)
        for i, a in enumerate((cb1, cb2))
        for n in range(2)
    ]
    c_tp = [local(a, tparams.at[i], 11 + i) for i, a in enumerate((tib, tg1, ts1, tg2, ts2, tb2))]
    c_ow = local(ow, wht, 17)
    c_q = [local(ob, obv, 18), local(qw, qwv, 19), local(qb, qbv, 20)]
    c_tiw = local(tiw, tiwv, 21)
    c_t = []
    for i, (src, dst) in enumerate(((tw1, w1r), (tw2, w2r))):
        for p in range(2):
            c_t.append(local(src, dst.at[:, pl.ds(p, 3), :, pl.ds(T * p, T)], 22 + 2 * i + p))

    def begin(copies):
        for c in copies:
            c.start()

    def finish(copies):
        for c in copies:
            c.wait()

    def lat_targets():
        for k in range(BACK + 1):
            for d in (-1, 0, 1):
                if k or d:
                    yield k, d

    def sends_to(k, d):
        ok = f + k < n_frames
        if d == -1:
            ok = jnp.logical_and(ok, rr > 0)
        if d == 1:
            ok = jnp.logical_and(ok, rr < n_rows - 1)
        return ok

    def gets_from(k, d):
        ok = f >= k
        if d == -1:
            ok = jnp.logical_and(ok, rr < n_rows - 1)
        if d == 1:
            ok = jnp.logical_and(ok, rr > 0)
        return ok

    c_vid.start()
    stbuf[...] = jnp.zeros(stbuf.shape, F32)
    tstbuf[...] = jnp.zeros(tstbuf.shape, F32)
    barrier = pltpu.get_barrier_semaphore()
    for d in range(1, n_rows):
        pl.semaphore_signal(
            barrier, inc=1, device_id={"frames": f, "rows": lax.rem(rr + d, n_rows)},
            device_id_type=MESH,
        )
    for k, d in lat_targets():
        if k:
            @pl.when(gets_from(k, d))
            def _():
                pl.semaphore_signal(
                    barrier, inc=1, device_id={"frames": f - k, "rows": rr - d}, device_id_type=MESH
                )

    begin(c_par + c_cb + c_tp + [c_ow] + c_q + [c_tiw])

    def halo(src_last, src_first, dst_above, dst_below, sem):
        down = pltpu.make_async_remote_copy(
            src_ref=src_last, dst_ref=dst_above, send_sem=sem.at[0], recv_sem=sem.at[1],
            device_id={"frames": f, "rows": rr + 1}, device_id_type=MESH,
        )
        up = pltpu.make_async_remote_copy(
            src_ref=src_first, dst_ref=dst_below, send_sem=sem.at[2], recv_sem=sem.at[3],
            device_id={"frames": f, "rows": rr - 1}, device_id_type=MESH,
        )
        return down, up

    has_above = rr > 0
    has_below = rr < n_rows - 1

    def stat_copies(buf, e):
        return [
            pltpu.make_async_remote_copy(
                src_ref=buf.at[rr], dst_ref=buf.at[rr],
                send_sem=st_sem.at[e, 0, d - 1], recv_sem=st_sem.at[e, 1, d - 1],
                device_id={"frames": f, "rows": lax.rem(rr + d, n_rows)}, device_id_type=MESH,
            )
            for d in range(1, n_rows)
        ]

    def send_stats(e, s, q):
        s = jnp.sum(s, axis=0, keepdims=True)
        q = jnp.sum(q, axis=0, keepdims=True)
        tiles = s.shape[1] // 128
        for t in range(tiles):
            stbuf[e, rr, t : t + 1, :] = s[:, 128 * t : 128 * t + 128]
            stbuf[e, rr, tiles + t : tiles + t + 1, :] = q[:, 128 * t : 128 * t + 128]
        copies = stat_copies(stbuf.at[e], e)
        begin(copies)
        return copies

    def norm_terms(e, copies, gain, shift):
        finish(copies)
        tiles = gain.shape[0]
        total = stbuf[e, 0]
        for r in range(1, n_rows):
            total = total + stbuf[e, r]
        total = lane_group_sum(total, C // GROUPS) * (1.0 / (n_rows * R * W * (C // GROUPS)))
        mean = total[0:tiles]
        var = jnp.maximum(total[tiles : 2 * tiles] - mean * mean, 0.0)
        scale = lax.rsqrt(var + EPS) * gain
        shift = shift - mean * scale
        wide = lambda x: jnp.concatenate([x[t : t + 1] for t in range(tiles)], axis=1) * 0.5
        return wide(scale), wide(shift)

    def put_line(line, v, scale, shift, halves=(0, 1), shifted=True):
        a = half_silu(v, scale, shift)
        taps = column_shifts(a) if shifted else (None, a.astype(BF16), None)
        for j, x in enumerate(taps):
            if x is not None:
                for n, half in enumerate(halves):
                    act[half, j, line] = x[:, HALF * n : HALF * n + HALF]

    def halo_lines(copies, above, below, scale, shift, halves=(0, 1), shifted=True):
        taps = range(3) if shifted else (1,)
        for has, copy, ref, line in (
            (has_above, copies[0], above, 0),
            (has_below, copies[1], below, R + 1),
        ):
            @pl.when(has)
            def _():
                copy.wait_recv()
                put_line(line, ref[...].astype(F32), scale, shift, halves, shifted)

            @pl.when(jnp.logical_not(has))
            def _():
                for half in halves:
                    for j in taps:
                        act[half, j, line] = jnp.zeros((W, HALF), BF16)

    def start_down(copies):
        @pl.when(has_below)
        def _():
            copies[0].start()

    def start_up(copies):
        @pl.when(has_above)
        def _():
            copies[1].start()

    def end_sends(copies):
        @pl.when(has_below)
        def _():
            copies[0].wait_send()

        @pl.when(has_above)
        def _():
            copies[1].wait_send()

    def conv(lhs_of, weight_of, width, finish_lines):
        def block(b, carry):
            s, q = carry
            lo = 2 * b
            hi = R - 2 - 2 * b
            acc = None
            for i in range(3):
                for j in range(3):
                    lhs = jnp.concatenate([lhs_of(j, lo + i), lhs_of(j, hi + i)], axis=0)
                    d = jnp.dot(lhs, weight_of(3 * i + j), preferred_element_type=F32)
                    acc = d if acc is None else acc + d
            return finish_lines(b, lo, hi, acc, s, q)

        zero = jnp.zeros((8, width), F32)
        return lax.fori_loop(0, 2, block, (zero, zero))

    def two_lines(half, j, line):
        return act[half, j, pl.ds(line, 2)].reshape(2 * W, HALF)

    c_vid.wait()
    begin(c_w1)

    def video_sums(r, carry):
        s, q = carry
        a, b = partial_sums(vid[r + 1].astype(F32))
        return s + a, q + b

    zero = jnp.zeros((8, C), F32)
    s, q = lax.fori_loop(0, R, video_sums, (zero, zero))

    later = sum(1 - lax.div(f + k, n_frames) for k in range(1, BACK + 1))
    lines = 2 + lax.div(rr + n_rows - 1, n_rows) - lax.div(rr + 1, n_rows)
    pl.semaphore_wait(barrier, n_rows - 1 + later * lines)

    copies = send_stats(0, s, q)
    vh = halo(vid.at[R], vid.at[1], vid.at[0], vid.at[R + 1], vh_sem)
    start_down(vh)
    start_up(vh)
    begin(c_w2)
    begin(c_t)

    finish([c_tiw])
    wbf[...] = jnp.zeros(wbf.shape, F32)
    for t in range(3):
        for j in range(3):
            for i in range(3):
                piece = tiwv[t, i, j].astype(F32)
                for n in range(R + 2):
                    top = SLOTS * j + packed_row(n + i - 2)
                    wbf[top : top + 4, T * n : T * n + T] = piece
        wb[256 * t : 256 * t + 256] = wbf[...].astype(BF16)

    finish(c_par + c_cb)
    scale, shift = norm_terms(0, copies, params[0], params[1])

    def video_line(r, _):
        put_line(r + 1, vid[r + 1].astype(F32), scale, shift)
        return 0

    lax.fori_loop(0, R, video_line, 0)
    halo_lines(vh, vid.at[0], vid.at[R + 1], scale, shift)
    finish(c_w1)

    hh = [halo(hsend.at[i, 1], hsend.at[i, 0], hrecv.at[i, 0], hrecv.at[i, 1], hh_sem.at[i]) for i in range(2)]

    def h_half(half, _):
        acc = None
        for i in range(3):
            for j in range(3):
                lhs = jnp.concatenate(
                    [act[n, j, i : i + R].reshape(R * W, HALF) for n in range(2)], axis=1
                )
                d = jnp.dot(lhs, w1[half, 3 * i + j], preferred_element_type=F32)
                acc = d if acc is None else acc + d
        v = acc + cbias[0, half]
        h[half] = v.reshape(R, W, HALF)
        hsend[half, 0] = v[:W].astype(BF16)
        hsend[half, 1] = v[R * W - W :].astype(BF16)
        copies = halo(
            hsend.at[half, 1], hsend.at[half, 0], hrecv.at[half, 0], hrecv.at[half, 1], hh_sem.at[half]
        )
        send_stats(1 + half, *partial_sums(v))
        start_down(copies)
        start_up(copies)
        return 0

    lax.fori_loop(0, 2, h_half, 0)

    def h_norm(half):
        scale, shift = norm_terms(
            1 + half, stat_copies(stbuf.at[1 + half], 1 + half), params[2, 2 * half : 2 * half + 2], params[3, 2 * half : 2 * half + 2]
        )

        def h_line(r, _):
            put_line(r + 1, h[half, r], scale, shift, (half,))
            return 0

        lax.fori_loop(0, R, h_line, 0)
        halo_lines(hh[half], hrecv.at[half, 0], hrecv.at[half, 1], scale, shift, (half,))

    h_norm(0)
    finish(c_w2)

    yh = [halo(ysend.at[i, 1], ysend.at[i, 0], yrecv.at[i, 0], yrecv.at[i, 1], yh_sem.at[i]) for i in range(2)]

    def y_part(b, lo, hi, acc, s, q):
        res = jnp.concatenate(
            [vid[pl.ds(lo + 1, 2)].reshape(2 * W, C), vid[pl.ds(hi + 1, 2)].reshape(2 * W, C)],
            axis=0,
        )
        v = res.astype(F32) + (acc + jnp.concatenate([cbias[1, 0], cbias[1, 1]], axis=1))
        for half in range(2):
            x = v[:, HALF * half : HALF * half + HALF]
            yp[half, pl.ds(lo, 2)] = x[: 2 * W].reshape(2, W, HALF)
            yp[half, pl.ds(hi, 2)] = x[2 * W :].reshape(2, W, HALF)
        return s, q

    conv(lambda j, line: two_lines(0, j, line), lambda tap: jnp.concatenate([w2[0, tap, 0:HALF], w2[1, tap, 0:HALF]], axis=1), C, y_part)

    h_norm(1)

    def y_half(half, _):
        acc = None
        for i in range(3):
            for j in range(3):
                lhs = act[1, j, i : i + R].reshape(R * W, HALF)
                d = jnp.dot(lhs, w2[half, 3 * i + j, HALF:C], preferred_element_type=F32)
                acc = d if acc is None else acc + d
        v = yp[half].reshape(R * W, HALF) + acc
        h[half] = v.reshape(R, W, HALF)
        ysend[half, 0] = v[:W].astype(BF16)
        ysend[half, 1] = v[R * W - W :].astype(BF16)
        copies = halo(
            ysend.at[half, 1], ysend.at[half, 0], yrecv.at[half, 0], yrecv.at[half, 1], yh_sem.at[half]
        )
        send_stats(3 + half, *partial_sums(v))
        start_down(copies)
        start_up(copies)
        return 0

    lax.fori_loop(0, 2, y_half, 0)

    finish([c_ow] + c_q + c_tp)
    nt = (((1,), (1,)), ((), ()))
    pt[...] = jnp.zeros(pt.shape, F32)
    for t in range(3):
        for dst in (w1r, w2r):
            dst[t, 3, :, 0:T] = jnp.zeros((3 * T, T), BF16)
            dst[t, 0, :, T : 2 * T] = jnp.zeros((3 * T, T), BF16)
    row = lax.broadcasted_iota(jnp.int32, (48, 8 * R), 0)
    col = lax.broadcasted_iota(jnp.int32, (48, 8 * R), 1)
    quant = jnp.zeros((48, 8 * R), F32)
    for m in range(8):
        for c in range(4):
            hit = (row % 5 == c) & (col % 8 == m) & (row // 5 == col // 8)
            quant = quant + jnp.where(hit, qwv[c : c + 1, m : m + 1], 0.0)
    row8 = lax.broadcasted_iota(jnp.int32, (8 * R, 1), 0)
    row5 = lax.broadcasted_iota(jnp.int32, (48, 1), 0)
    head_bias = jnp.zeros((8 * R, 1), F32)
    for m in range(8):
        head_bias = head_bias + jnp.where(row8 % 8 == m, obv[0:1, m : m + 1], 0.0)
    quant_bias = jnp.zeros((48, 1), F32)
    for c in range(4):
        quant_bias = quant_bias + jnp.where(row5 % 5 == c, qbv[0:1, c : c + 1], 0.0)

    def y_norm(half):
        scale, shift = norm_terms(
            3 + half, stat_copies(stbuf.at[3 + half], 3 + half),
            params[4, 2 * half : 2 * half + 2], params[5, 2 * half : 2 * half + 2],
        )

        def y_line(r, _):
            put_line(r + 1, h[half, r], scale, shift, (half,), shifted=False)
            return 0

        lax.fori_loop(0, R, y_line, 0)
        halo_lines(yh[half], yrecv.at[half, 0], yrecv.at[half, 1], scale, shift, (half,), shifted=False)

    y_norm(0)
    for r in range(R + 2):
        pt[r, :, 0:W] = lax.dot_general(wht[:, 0:HALF], act[0, 1, r], nt, preferred_element_type=F32)
    y_norm(1)
    for r in range(R + 2):
        pt[r, :, 0:W] += lax.dot_general(wht[:, HALF:C], act[1, 1, r], nt, preferred_element_type=F32)
    for r in range(R):
        sums = []
        for j in range(3):
            x = None
            for i in range(3):
                top = 8 * (3 * i + j)
                p = pt[r + i, top : top + 8, :]
                x = p if x is None else x + p
            sums.append(x)
        mom[8 * r : 8 * r + 8] = (
            sums[1] + pltpu.roll(sums[0], 1, 1) + pltpu.roll(sums[2], LANES - 1, 1)
        )
    means = (
        jnp.dot(quant, mom[...] + head_bias, precision=lax.Precision.HIGHEST, preferred_element_type=F32)
        + quant_bias
    )
    means = LATENT_SCALE * means
    row = lax.broadcasted_iota(jnp.int32, (48, 128), 0)
    lane = lax.broadcasted_iota(jnp.int32, (48, 128), 1)
    rest = jnp.where((lane < W - 128) & (row < 5 * R), means[:, 128:256], 0.0)
    packed = jnp.where(row % 5 < 4, means[:, 0:128], 0.0)
    for c in range(4):
        moved = pltpu.roll(jnp.where(row % 5 == c, rest, 0.0), 4 - c, 0)
        packed = packed + (pltpu.roll(moved, 32 * c, 1) if c else moved)
    packed = jnp.where(row < 5 * R, packed, 0.0)
    latsend[0:48] = packed.astype(BF16)
    latsend[48:64] = pltpu.roll(packed, 48 - 25, 0)[0:16].astype(BF16)
    lx[0, 16:64] = packed.astype(BF16)

    def lat_copy(k, d):
        src = {0: pl.ds(0, 48), 1: pl.ds(48, 16), -1: pl.ds(0, 16)}[d]
        at = {0: pl.ds(16, 48), 1: pl.ds(0, 16), -1: pl.ds(64, 16)}[d]
        return pltpu.make_async_remote_copy(
            src_ref=latsend.at[src], dst_ref=lx.at[k, at],
            send_sem=lat_send.at[k, d + 1], recv_sem=lat_recv.at[k, d + 1],
            device_id={"frames": f + k, "rows": rr + d}, device_id_type=MESH,
        )

    for k, d in lat_targets():
        @pl.when(sends_to(k, d))
        def _():
            lat_copy(k, d).start()

    slot = lax.broadcasted_iota(jnp.int32, (SLOTS, 128), 0)
    lowest = jnp.where(has_above, 0, 16)
    highest = jnp.where(has_below, SLOTS, 64)
    column = lax.broadcasted_iota(jnp.int32, (W, 128), 0)
    lane = lax.broadcasted_iota(jnp.int32, (W, 128), 1)
    lane32 = lax.broadcasted_iota(jnp.int32, (32, 128), 1)
    fifth = lane32 < 0
    for line in range(-3, R + 3):
        fifth = fifth | (lane32 == packed_row(line) + 4)

    def take_latent(k, dirs=(-1, 0, 1)):
        for d in dirs:
            @pl.when(gets_from(k, d))
            def _():
                lat_copy(k, d).wait_recv()
        keep = (slot >= jnp.where(f >= k, lowest, SLOTS)) & (slot < highest)
        x = jnp.where(keep, lx[k].astype(F32), 0.0)
        x = jnp.transpose(jnp.concatenate([x, jnp.zeros((128 - SLOTS, 128), F32)], axis=0))
        rest = jnp.zeros((32, 128), F32)
        for c in range(4):
            rest = rest + pltpu.roll(jnp.where(fifth, x[32 * c : 32 * c + 32], 0.0), 128 + c - 4, 1)
        x = jnp.concatenate([x, rest], axis=0)
        left = jnp.where(column == 0, 0.0, pltpu.roll(x, 1, 0))
        right = jnp.where(column == W - 1, 0.0, pltpu.roll(x, W - 1, 0))
        centre = pltpu.roll(x, SLOTS, 1)
        ltt[k, :, 0:128] = jnp.where(lane < SLOTS, left, centre).astype(BF16)
        ltt[k, :, 128:256] = jnp.where(lane < 2 * SLOTS - 128, centre, pltpu.roll(right, 2 * SLOTS - 128, 1)).astype(BF16)

    def send_time_stats(e, s, q):
        tstbuf[e, rr, 0:1] = jnp.sum(s, axis=0, keepdims=True)
        tstbuf[e, rr, 1:2] = jnp.sum(q, axis=0, keepdims=True)
        begin(stat_copies(tstbuf.at[e], 5 + e))

    def time_terms(e, gain, shift):
        finish(stat_copies(tstbuf.at[e], 5 + e))
        total = tstbuf[e, 0]
        for r in range(1, n_rows):
            total = total + tstbuf[e, r]
        total = lane_group_sum(total, T // GROUPS) * (1.0 / (n_rows * R * W * (T // GROUPS)))
        mean = total[0:1]
        var = jnp.maximum(total[1:2] - mean * mean, 0.0)
        scale = lax.rsqrt(var + EPS) * gain
        return 0.5 * scale, 0.5 * (shift - mean * scale)

    def time_line(dst, g, n, v, scale, shift):
        for j, x in enumerate(column_shifts(half_silu(v, scale, shift))):
            dst[g, n, :, T * j : T * j + T] = x

    def pair_lines(src, g, i, pairs):
        return jnp.concatenate([src[g, 2 * p + i] for p in range(pairs)], axis=0)

    take_latent(0, (-1, 1))
    take_latent(1)

    def t0_frame(g, _):
        take_latent(g + 2)
        lhs = jnp.concatenate([ltt[g + 2], ltt[g + 1], ltt[g]], axis=1)
        s = jnp.zeros((8, T), F32)
        q = jnp.zeros((8, T), F32)
        acc = jnp.dot(lhs, wb[...], preferred_element_type=F32)
        for n in range(R + 2):
            v = acc[:, T * n : T * n + T] + tparams[0]
            t0s[g, n] = v
            if 1 <= n < R + 1:
                a, c = partial_sums(v)
                s += a
                q += c
        send_time_stats(g, s, q)
        return 0

    lax.fori_loop(0, 5, t0_frame, 0)

    finish(c_t)

    def b1_frame(g):
        scale, shift = time_terms(g, tparams[1], tparams[2])

        def lines(m, _):
            for n in [5 * m + i for i in range(5)]:
                at = R * rr + n - 1
                ok = jnp.logical_and(jnp.logical_and(at >= 0, at < n_rows * R), f >= g)
                time_line(b1, g, n, t0s[g, n], jnp.where(ok, scale, 0.0), jnp.where(ok, shift, 0.0))
            return 0

        lax.fori_loop(0, (R + 2) // 5, lines, 0)

    def b1_first(g, _):
        b1_frame(g)
        return 0

    lax.fori_loop(0, 2, b1_first, 0)

    pairs = R // 2

    def th(g):
        return halo(
            t1send.at[g, 1], t1send.at[g, 0], t1recv.at[g, 0], t1recv.at[g, 1], th_sem.at[g]
        )

    def t1_frame(g, _):
        b1_frame(g + 2)
        lhs = jnp.concatenate(
            [pair_lines(b1, g + 2 - t, i, pairs) for t in range(3) for i in range(4)], axis=1
        )
        acc = jnp.dot(lhs, w1r[...].reshape(12 * 3 * T, 2 * T), preferred_element_type=F32)
        s = jnp.zeros((8, T), F32)
        q = jnp.zeros((8, T), F32)
        for p in range(pairs):
            for half in range(2):
                v = acc[W * p : W * p + W, T * half : T * half + T]
                t1s[g, 2 * p + half] = v
                if 2 * p + half in (0, R - 1):
                    t1send[g, half] = v.astype(BF16)
                a, c = partial_sums(v)
                s += a
                q += c
        send_time_stats(5 + g, s, q)
        start_down(th(g))
        start_up(th(g))
        return 0

    lax.fori_loop(0, 3, t1_frame, 0)

    for p in range(R // 2):
        for half in range(2):
            facc[W * p : W * p + W, T * half : T * half + T] = t0s[0, 2 * p + half + 1] + tparams[5]

    def feature_frame(g, _):
        scale, shift = time_terms(5 + g, tparams[3], tparams[4])
        scale = jnp.where(f >= g, scale, 0.0)
        shift = jnp.where(f >= g, shift, 0.0)

        def lines(m, _):
            for n in [4 * m + i for i in range(4)]:
                time_line(b2, g, n + 1, t1s[g, n], scale, shift)
            return 0

        lax.fori_loop(0, R // 4, lines, 0)
        for has, copy, side, n in ((has_above, th(g)[0], 0, 0), (has_below, th(g)[1], 1, R + 1)):
            @pl.when(has)
            def _():
                copy.wait_recv()
                time_line(b2, g, n, t1recv[g, side].astype(F32), scale, shift)

            @pl.when(jnp.logical_not(has))
            def _():
                b2[g, n] = jnp.zeros((W, 3 * T), BF16)

        lhs = jnp.concatenate([pair_lines(b2, g, i, R // 2) for i in range(4)], axis=1)
        facc[...] += jnp.dot(
            lhs, w2r[2 - g].reshape(4 * 3 * T, 2 * T), preferred_element_type=F32
        )
        return 0

    lax.fori_loop(0, 3, feature_frame, 0)

    for p in range(R // 2):
        for half in range(2):
            out[2 * p + half] = facc[W * p : W * p + W, T * half : T * half + T].astype(BF16)
    end_sends(vh)
    end_sends(hh[0])
    end_sends(hh[1])
    end_sends(yh[0])
    end_sends(yh[1])
    for g in range(3):
        end_sends(th(g))
    for k, d in lat_targets():
        @pl.when(sends_to(k, d))
        def _():
            lat_copy(k, d).wait_send()


def body(
    video, norm1_gain, norm1_shift, conv1_weight, conv1_bias, norm2_gain, norm2_shift,
    conv2_weight, conv2_bias, out_gain, out_shift, out_weight, out_bias, quant_weight,
    quant_bias, time_in_weight, time_in_bias, tnorm1_gain, tnorm1_shift, time1_weight,
    tnorm2_gain, tnorm2_shift, time2_weight, time2_bias, *, n_frames, n_rows,
):
    tile = lambda a: a.reshape(4, 128)
    flat = lambda a: a.reshape(1, -1)
    args = (
        video.reshape(R, W, C),
        tile(norm1_gain), tile(norm1_shift), conv1_weight.reshape(9, C, C), flat(conv1_bias),
        tile(norm2_gain), tile(norm2_shift), conv2_weight.reshape(9, C, C), flat(conv2_bias),
        tile(out_gain), tile(out_shift), out_weight.transpose(0, 1, 3, 2).reshape(72, C), flat(out_bias),
        quant_weight.T, flat(quant_bias), time_in_weight, flat(time_in_bias),
        flat(tnorm1_gain), flat(tnorm1_shift), time1_weight.reshape(3, 3, 3 * T, T),
        flat(tnorm2_gain), flat(tnorm2_shift), time2_weight.reshape(3, 3, 3 * T, T),
        flat(time2_bias),
    )
    vmem = lambda *shape, dtype=BF16: pltpu.VMEM(shape, dtype)
    dma = pltpu.SemaphoreType.DMA
    result = pl.pallas_call(
        functools.partial(kernel, n_frames, n_rows),
        out_shape=pltpu.VMEM((R, W, T), BF16),
        in_specs=[pl.BlockSpec(memory_space=pl.ANY)] * len(args),
        out_specs=pl.BlockSpec(memory_space=pltpu.VMEM),
        scratch_shapes=[
            vmem(R + 2, W, C),
            vmem(2, 9, C, HALF),
            vmem(2, 9, C, HALF),
            vmem(2, 3, R + 2, W, HALF),
            vmem(2, R, W, HALF, dtype=F32),
            vmem(2, R, W, HALF, dtype=F32),
            vmem(2, 2, W, HALF),
            vmem(2, 2, W, HALF),
            vmem(2, 2, W, HALF),
            vmem(2, 2, W, HALF),
            vmem(6, 4, 128, dtype=F32),
            vmem(2, 2, 1, HALF, dtype=F32),
            vmem(6, 1, T, dtype=F32),
            vmem(1, 8, dtype=F32),
            vmem(4, 8, dtype=F32),
            vmem(1, 4, dtype=F32),
            vmem(3, 3, 3, 4, T),
            vmem(72, C),
            vmem(R + 2, 72, LANES, dtype=F32),
            vmem(8 * R, LANES, dtype=F32),
            vmem(256, (R + 2) * T, dtype=F32),
            vmem(768, (R + 2) * T),
            vmem(3, 4, 3 * T, 2 * T),
            vmem(3, 4, 3 * T, 2 * T),
            vmem(5, n_rows, 8, 128, dtype=F32),
            vmem(8, n_rows, 8, 128, dtype=F32),
            vmem(64, 128),
            vmem(BACK + 1, SLOTS, 128),
            vmem(BACK + 1, W, 256),
            vmem(5, R + 2, W, T, dtype=F32),
            vmem(5, R + 2, W, 3 * T),
            vmem(3, R, W, T, dtype=F32),
            vmem(3, 2, W, T),
            vmem(3, 2, W, T),
            vmem(3, R + 2, W, 3 * T),
            vmem(R // 2 * W, 2 * T, dtype=F32),
            dma((30,)),
            dma((4,)),
            dma((2, 4)),
            dma((2, 4)),
            dma((3, 4)),
            dma((13, 2, n_rows - 1)),
            dma((BACK + 1, 3)),
            dma((BACK + 1, 3)),
        ],
        compiler_params=pltpu.CompilerParams(
            collective_id=0, has_side_effects=True, vmem_limit_bytes=60 * 1024 * 1024
        ),
        name="encoder_window",
    )(*args)
    return result[None]


def solution(mesh):
    step = functools.partial(body, n_frames=mesh.shape["frames"], n_rows=mesh.shape["rows"])
    return jax.shard_map(
        step,
        mesh=mesh,
        in_specs=(P("frames", "rows", None, None),) + (P(),) * 23,
        out_specs=P("frames", "rows", None, None),
        check_vma=False,
    )
```
